32 devices in a mesh: gx: 4 (over x, core), gy: 2 (over y), gz: 4 (over z).
Axes of the slice: x: 2, y: 2, z: 4, core: 2. Of those that a mesh axis runs over, the one named last changes fastest.
Arguments:
- offsets: float32 [3, 4, 4, 8, 128], P(None, 'gx', 'gy', 'gz'), may hold values from 0 to 11, as said below
- type_ids: int32 [4, 4, 8, 128], P('gx', 'gy', 'gz'), may hold values from 0 to 1
- neighbours: int32 [4, 4, 8, 27], P('gx', 'gy', 'gz'), may hold values from 0 to 48, as said below
- type_chi: float32 [2], replicated, may hold values from 3 to 7
- type_eta: float32 [2], replicated, may hold values from 6 to 12
- type_gamma: float32 [2], replicated, may hold values from 0.5 to 1
Outputs:
- charges: float32 [4, 4, 8, 128], P('gx', 'gy', 'gz')
- residuals: float32 [2, 4, 4, 8, 128], P(None, 'gx', 'gy', 'gz')
The draws below stay inside these ranges and needn't reach their ends.
Inputs may be any that keep to these rules, and one draw needn't show every extreme that they name: `neighbours`: each tile's row lists the tile itself and some of the 26 cells around it, each at most once, as indices into its device's block padded by one cell on every side (3) x (4) x (4) in first-dimension-major order; unused slots hold (3) * 4 * 4. Two tiles list each other with opposite displacements or not at all. `offsets`: any two atoms of the box lie at least 0.8 A apart.
All inputs are finite; a program needn't handle non-finite values.
Results may differ from the reference program's by a relative error of at most 0.0003.
Values sent between devices are 32-bit elements; how exact they have to be, the bound alone decides.
A program may use at most 64 MiB of HBM per device.

```python
import jax
import jax.numpy as jnp
import numpy as np
from jax import lax

ATOMS = 128
NB = 27
TYPES = 2
ITERS = 3
CX = 1
CY = 2
CZ = 2
NCX = 4
NCY = 4
NCZ = 8


def lattice_sites():
    side = 1
    while (side + 1) ** 3 <= ATOMS:
        side = side + 1
    spacing = 11.0 / side
    points = []
    for first_step in range(side):
        for second_step in range(side):
            for third_step in range(side):
                points.append([(first_step + 0.5) * spacing, (second_step + 0.5) * spacing, (third_step + 0.5) * spacing])
    inner = max(side - 1, 1)
    extra_count = ATOMS - side ** 3
    for extra_index in range(extra_count):
        first_step = extra_index // (inner * inner)
        second_step = extra_index // inner % inner
        third_step = extra_index % inner
        points.append([spacing, spacing, (third_step + 1.0) * spacing])
    return np.array(points, dtype=np.float32).T


def draw_offsets(key, part):
    base = jnp.asarray(lattice_sites())[:, None, None, None, :]
    jitter = jnp.clip(0.12 * jax.random.normal(key, (3, NCX, NCY, NCZ, ATOMS), jnp.float32), -0.3, 0.3)
    return jnp.clip(base + jitter, 0.0, 10.999).astype(jnp.float32)


def draw_neighbours(key, part):
    offset_table = np.array([[first_step, second_step, third_step] for first_step in (-1, 0, 1) for second_step in (-1, 0, 1) for third_step in (-1, 0, 1)], dtype=np.int32)
    keep_bits = jax.random.randint(key, (NCX, NCY, NCZ, 13), 0, 4) > 0
    columns = []
    for slot_index in range(27):
        if slot_index < 13:
            columns.append(keep_bits[..., slot_index])
        elif slot_index == 13:
            columns.append(jnp.ones((NCX, NCY, NCZ), dtype=bool))
        else:
            mirror = 26 - slot_index
            moved = offset_table[slot_index]
            columns.append(jnp.roll(keep_bits[..., mirror], shift=(-int(moved[0]), -int(moved[1]), -int(moved[2])), axis=(0, 1, 2)))
    kept = jnp.stack(columns, -1)
    local_one = (jnp.arange(NCX, dtype=jnp.int32) % CX)[:, None, None, None]
    local_two = (jnp.arange(NCY, dtype=jnp.int32) % CY)[None, :, None, None]
    local_three = (jnp.arange(NCZ, dtype=jnp.int32) % CZ)[None, None, :, None]
    table_one = jnp.asarray(offset_table[:, 0])[None, None, None, :]
    table_two = jnp.asarray(offset_table[:, 1])[None, None, None, :]
    table_three = jnp.asarray(offset_table[:, 2])[None, None, None, :]
    padded_index = ((local_one + 1 + table_one) * (CY + 2) + (local_two + 1 + table_two)) * (CZ + 2) + (local_three + 1 + table_three)
    padded_index = jnp.broadcast_to(padded_index, (NCX, NCY, NCZ, 27))
    sentinel = (CX + 2) * (CY + 2) * (CZ + 2)
    slot_order = jnp.arange(27, dtype=jnp.int32)[None, None, None, :]
    order_key = jnp.where(kept, slot_order, slot_order + 27)
    order = jnp.argsort(order_key, axis=-1, stable=True)
    index_sorted = jnp.take_along_axis(padded_index, order, -1)
    kept_sorted = jnp.take_along_axis(kept, order, -1)
    return jnp.where(kept_sorted, index_sorted, sentinel).astype(jnp.int32)


def touch_ends(values, stream_key, least, top_value):
    shape = values.shape
    spot = [jax.random.randint(jax.random.fold_in(stream_key, axis), (), 0, shape[axis]) for axis in range(len(shape))]
    values = values.at[tuple(spot)].set(least)
    longest = shape.index(max(shape))
    spot[longest] = (spot[longest] + 1) % shape[longest]
    return values.at[tuple(spot)].set(top_value)


def setup_inputs(seed: int = 0) -> dict:
    arg_keys = jax.random.split(jax.random.key(seed), 7)
    return {
        "offsets": draw_offsets(jax.random.fold_in(arg_keys[6], 71), 0),
        "type_ids": touch_ends(jax.random.randint(arg_keys[1], (NCX, NCY, NCZ, ATOMS), 0, TYPES), jax.random.fold_in(arg_keys[1], 1), 0, TYPES - 1).astype(jnp.int32),
        "neighbours": draw_neighbours(jax.random.fold_in(arg_keys[6], 71), 0),
        "type_chi": jnp.clip(jax.random.uniform(arg_keys[3], (TYPES,), jnp.float32, 3.0, 7.0), 3.0, 7.0),
        "type_eta": jnp.clip(jax.random.uniform(arg_keys[4], (TYPES,), jnp.float32, 6.0, 12.0), 6.0, 12.0),
        "type_gamma": jnp.clip(jax.random.uniform(arg_keys[5], (TYPES,), jnp.float32, 0.5, 1.0), 0.5, 1.0),
    }


CELL_EDGE = 11.0
CUTOFF = 10.0
COULOMB = 14.4

def taper_value(distance):
    scaled = distance / CUTOFF
    squared = scaled * scaled
    return 1.0 + squared * squared * (-35.0 + scaled * (84.0 + scaled * (-70.0 + scaled * 20.0)))

def couplings(own_pos, own_shield, near_pos, near_shield, shifts, listed, itself):
    displace = near_pos[:, :, None, :] + shifts[:, :, None, None] - own_pos[:, None, :, None]
    dist_sq = lax.optimization_barrier(jnp.sum(displace * displace, axis=0))
    distance = jnp.sqrt(dist_sq)
    screen = own_shield[None, :, None] * near_shield[:, None, :]
    kernel = COULOMB * taper_value(distance) / jnp.cbrt(dist_sq * distance + screen)
    diagonal_mask = jnp.eye(own_pos.shape[1], dtype=bool)
    retained = listed[:, None, None] & (distance < CUTOFF) & jnp.logical_not(itself[:, None, None] & diagonal_mask[None])
    return jnp.where(retained, kernel, jnp.zeros_like(kernel))

def table_lookup(type_ids, table):
    result = jnp.zeros(type_ids.shape, table.dtype)
    for kind_index in range(table.shape[0]):
        result = jnp.where(type_ids == kind_index, table[kind_index], result)
    return result

def decode_cells(entries, local_one, local_two, local_three, width_two, width_three):
    plane_cells = (width_two + 2) * (width_three + 2)
    step_one = entries // plane_cells - 1 - local_one[..., None]
    step_two = entries // (width_three + 2) % (width_two + 2) - 1 - local_two[..., None]
    step_three = entries % (width_three + 2) - 1 - local_three[..., None]
    return (step_one, step_two, step_three)

def reference(offsets, type_ids, neighbours, type_chi, type_eta, type_gamma):
    tiles = NCX * NCY * NCZ
    sentinel = (CX + 2) * (CY + 2) * (CZ + 2)
    shape_grid = (NCX, NCY, NCZ)
    grid_one = jnp.broadcast_to(jnp.arange(NCX, dtype=jnp.int32)[:, None, None], shape_grid)
    grid_two = jnp.broadcast_to(jnp.arange(NCY, dtype=jnp.int32)[None, :, None], shape_grid)
    grid_three = jnp.broadcast_to(jnp.arange(NCZ, dtype=jnp.int32)[None, None, :], shape_grid)
    step_one, step_two, step_three = decode_cells(neighbours, grid_one % CX, grid_two % CY, grid_three % CZ, CY, CZ)
    listed = neighbours != sentinel
    itself = (step_one == 0) & (step_two == 0) & (step_three == 0)
    target = ((grid_one[..., None] + step_one) % NCX * NCY + (grid_two[..., None] + step_two) % NCY) * NCZ + (grid_three[..., None] + step_three) % NCZ
    target = jnp.where(listed, target, tiles).astype(jnp.int32).reshape(tiles, NB)
    shifts = jnp.stack([step_one, step_two, step_three], axis=-2).reshape(tiles, 3, NB).astype(jnp.float32) * CELL_EDGE
    listed = listed.reshape(tiles, NB)
    itself = itself.reshape(tiles, NB)
    chi_atom = table_lookup(type_ids, type_chi).reshape(tiles, ATOMS)
    eta_atom = table_lookup(type_ids, type_eta).reshape(tiles, ATOMS)
    shield = table_lookup(type_ids, type_gamma ** (-1.5)).reshape(tiles, ATOMS)
    positions = offsets.reshape(3, tiles, ATOMS)
    pos_all = jnp.concatenate([positions, jnp.zeros((3, 1, ATOMS), positions.dtype)], 1)
    shield_all = jnp.concatenate([shield, jnp.zeros((1, ATOMS), shield.dtype)], 0)
    own_pos = jnp.moveaxis(positions, 1, 0)
    batch_size = 16
    rounds = tiles // batch_size

    def grouped(stacked):
        return stacked.reshape((rounds, batch_size) + stacked.shape[1:])
    inputs = (grouped(own_pos), grouped(shield), grouped(target), grouped(shifts), grouped(listed), grouped(itself))
    build_batch = jax.vmap(couplings)

    def tile_pass(vectors):
        padded = jnp.concatenate([vectors, jnp.zeros((2, 1, ATOMS), vectors.dtype)], 1)

        def one_round(tile_item):
            own_block, own_screen, row_index, shifted, valid_slot, selfish = tile_item
            near_block = jnp.moveaxis(pos_all[:, row_index], 0, 1)
            near_screen = shield_all[row_index]
            blocks = build_batch(own_block, own_screen, near_block, near_screen, shifted, valid_slot, selfish)
            values = padded[:, row_index]
            return jnp.einsum('bsij,cbsj->cbi', blocks, values, precision=lax.Precision.HIGHEST)
        products = lax.map(one_round, inputs)
        return jnp.moveaxis(products, 1, 0).reshape(2, tiles, ATOMS)
    source = jnp.stack([-chi_atom, -jnp.ones_like(chi_atom)])
    diagonal = eta_atom
    solution = jnp.zeros_like(source)
    residual = source
    direction = source
    norm_now = lax.optimization_barrier(jnp.sum(residual * residual, axis=(1, 2)))
    for iteration in range(ITERS):
        coupled = tile_pass(direction)
        image_now = diagonal[None] * direction + coupled
        step_size = norm_now / lax.optimization_barrier(jnp.sum(direction * image_now, axis=(1, 2)))
        solution = solution + step_size[:, None, None] * direction
        residual = residual - step_size[:, None, None] * image_now
        norm_next = lax.optimization_barrier(jnp.sum(residual * residual, axis=(1, 2)))
        direction = residual + (norm_next / norm_now)[:, None, None] * direction
        norm_now = norm_next
    level_ratio = jnp.sum(solution[0]) / jnp.sum(solution[1])
    charges = (1000.0 * (solution[0] - level_ratio * solution[1])).reshape(NCX, NCY, NCZ, ATOMS)
    return (charges, residual.reshape(2, NCX, NCY, NCZ, ATOMS))
```

```python
import itertools

import jax
import jax.numpy as jnp
from jax import lax
from jax.experimental import pallas as pl
from jax.experimental.pallas import tpu as pltpu
from jax.sharding import PartitionSpec as P

ITERS = 3
CELL_EDGE = 11.0
CUTOFF = 10.0
COULOMB = 14.4
AXES = ("gx", "gy", "gz")
FAR = 1000.0
MESH = pl.DeviceIdType.MESH
STEPS = [d for d in itertools.product((-1, 0, 1), repeat=3)]
REMOTE = sorted((d for d in STEPS if d != (0, 0, 0)), key=lambda d: (-abs(d[2]), -abs(d[0])))
KINDS = 3


def kind_of(step):
    return 2 if step[2] else (1 if step[0] else 0)


def rounded_sides(step, cells):
    source, target = [], []
    for d, c in zip(step, cells):
        if d == 0:
            source.append(pl.ds(1, c))
            target.append(pl.ds(1, c))
        elif d > 0:
            source.append(pl.ds(c, 1))
            target.append(pl.ds(0, 1))
        else:
            source.append(pl.ds(1, 1))
            target.append(pl.ds(c + 1, 1))
    return tuple(source), tuple(target)


def make_kernel(sizes, groups, cells, atoms, types, rows):
    width = tuple(c + 2 for c in cells)
    tiles = cells[0] * cells[1] * cells[2]
    local = list(itertools.product(*[range(c) for c in cells]))
    padded = list(itertools.product(*[range(w) for w in width]))
    own = tuple(slice(1, 1 + c) for c in cells)
    group_sizes = []
    for axes in groups:
        count = 1
        for a in axes:
            count = count * sizes[a]
        group_sizes.append(count)
    boxes = (
        (pl.ds(0, cells[0]), pl.ds(0, 2), pl.ds(0, cells[2])),
        (pl.ds(0, 2), pl.ds(0, width[1]), pl.ds(0, cells[2])),
        (pl.ds(0, width[0]), pl.ds(0, width[1]), pl.ds(0, 2)),
    )

    def linear(place):
        return (place[0] * width[1] + place[1]) * width[2] + place[2]

    def reach(place):
        if not 1 <= place[2] <= cells[2]:
            return 2
        return 0 if all(1 <= p <= c for p, c in zip(place, cells)) else 1

    pairs = [[], [], []]
    for t, home in enumerate(local):
        split = [[], [], []]
        for n, step in enumerate(STEPS):
            place = tuple(h + 1 + d for h, d in zip(home, step))
            split[reach(place)].append((n, place))
        for kept, part in zip(pairs, split):
            kept.append((t, part))

    def kernel(*refs):
        hbm, (charge_ref, resid_ref) = refs[:6], refs[6:8]
        (off_ref, type_ref, list_ref, chi_ref, eta_ref, gamma_ref) = refs[8:14]
        (fields, geometry, columns, listed, blocks, sums, source, first, second, own_image) = refs[14:24]
        parts = refs[24 : 24 + len(groups)]
        load_sem, halo_send, halo_recv, sum_send, sum_recv = refs[24 + len(groups) :]

        loads = [
            pltpu.make_async_copy(a, b, load_sem.at[k])
            for k, (a, b) in enumerate(
                zip(hbm, (off_ref, type_ref, list_ref, chi_ref, eta_ref, gamma_ref))
            )
        ]
        for load in loads:
            load.start()

        me = {a: lax.axis_index(a) for a in AXES}

        def neighbour(step):
            return tuple(
                lax.rem(me[a] + (d + sizes[a]), sizes[a]) for a, d in zip(AXES, step)
            )

        def member(axes, hop):
            rank = 0
            count = 1
            for a in axes:
                rank = rank * sizes[a] + me[a]
                count = count * sizes[a]
            rank = lax.rem(rank + hop, count)
            place = dict(me)
            for a in reversed(axes):
                place[a] = lax.rem(rank, sizes[a])
                rank = rank // sizes[a]
            return tuple(place[a] for a in AXES)

        def lookup(kinds, table):
            result = jnp.zeros(kinds.shape, jnp.float32)
            for k in range(types):
                result = jnp.where(kinds == float(k), table[k], result)
            return result

        barrier = pltpu.get_barrier_semaphore()
        greeted = 0
        for axes, count in zip(groups, group_sizes):
            for hop in range(1, count):
                pl.semaphore_signal(
                    barrier, inc=1, device_id=member(axes, hop), device_id_type=MESH
                )
                greeted += 1
        if len(groups) > 1:
            for step in REMOTE:
                pl.semaphore_signal(
                    barrier, inc=1, device_id=neighbour(step), device_id_type=MESH
                )
                greeted += 1

        for load in loads:
            load.wait()

        def tenth(values, f, place):
            return (values + CELL_EDGE * (place[f] - 1.0)) * (1.0 / CUTOFF)

        def sigma(kinds):
            root = lax.rsqrt(lookup(kinds, gamma_ref))
            return root * root * root * (CUTOFF**-1.5)

        for x, y, z in local:
            for f in range(3):
                fields[x + 1, y + 1, z + 1, f : f + 1, :] = off_ref[f, x, y, z : z + 1, :]
            fields[x + 1, y + 1, z + 1, 3:4, :] = type_ref[x, y, z : z + 1, :].astype(jnp.float32)

        def locate(places):
            for x, y, z in places:
                place = (x, y, z)
                kinds = fields[x, y, z, 3:4, :]
                for f in range(3):
                    geometry[x, y, z, f : f + 1, :] = tenth(fields[x, y, z, f : f + 1, :], f, place)
                geometry[x, y, z, 3:4, :] = sigma(kinds)
                source[x, y, z, 0:1, :] = -lookup(kinds, chi_ref)
                source[x, y, z, 1:2, :] = jnp.full((1, atoms), -1.0, jnp.float32)

        locate([p for p in padded if reach(p) == 0])
        for t, (x, y, z) in enumerate(local):
            for f in range(4):
                row = geometry[x + 1, y + 1, z + 1, f : f + 1, :]
                columns[t, f] = jnp.transpose(jnp.broadcast_to(row, (atoms, atoms)))
        entries = jnp.concatenate(
            [list_ref[x, y, z : z + 1, :] - linear((x + 1, y + 1, z + 1)) for x, y, z in local], 0
        )
        for n, step in enumerate(STEPS):
            found = jnp.max(
                jnp.where(entries == linear(step), 1.0, 0.0), axis=1, keepdims=True
            )
            listed[n] = jnp.broadcast_to(1.0 - (1.0 - found) * FAR, (tiles, atoms))
        eta = [lookup(fields[x + 1, y + 1, z + 1, 3:4, :], eta_ref) for x, y, z in local]

        with jax.named_scope("barrier"):
            pl.semaphore_wait(barrier, greeted)

        def halo(buffer, stage):
            for step in REMOTE:
                here, there = rounded_sides(step, cells)
                kind = kind_of(step)
                pltpu.make_async_remote_copy(
                    src_ref=buffer.at[here],
                    dst_ref=buffer.at[there],
                    send_sem=halo_send.at[stage, kind],
                    recv_sem=halo_recv.at[stage, kind],
                    device_id=neighbour(step),
                    device_id_type=MESH,
                ).start()

        def whole_kind(buffer, stage, kind):
            return pltpu.make_async_remote_copy(
                src_ref=buffer.at[boxes[kind]],
                dst_ref=buffer.at[boxes[kind]],
                send_sem=halo_send.at[stage, kind],
                recv_sem=halo_recv.at[stage, kind],
                device_id=neighbour(REMOTE[0]),
                device_id_type=MESH,
            )

        def arrived(buffer, stage, which):
            if which == 1:
                whole_kind(buffer, stage, 0).wait_recv()
                whole_kind(buffer, stage, 1).wait_recv()
            if which == 2:
                whole_kind(buffer, stage, 2).wait_recv()

        slabs = atoms // rows

        def coupling(t, n, place, at, own_part):
            near = [geometry[place[0], place[1], place[2], f : f + 1, :] for f in range(4)]
            dx = near[0] - own_part[0]
            dy = near[1] - own_part[1]
            dz = near[2] - own_part[2]
            square = dx * dx + dy * dy + dz * dz
            if STEPS[n] == (0, 0, 0):
                i = lax.broadcasted_iota(jnp.int32, (rows, atoms), 0) + at
                j = lax.broadcasted_iota(jnp.int32, (rows, atoms), 1)
                square = jnp.where(i == j, 4.0, square)
            u = square * lax.rsqrt(square)
            w = jnp.maximum(listed[n, t : t + 1, :] - u, 0.0)
            w = w * w
            w = w * w
            shape = (u + 0.5) * (square + 0.2) - 0.05
            cube = square * u + own_part[3] * near[3]
            return w * shape * jnp.exp2(jnp.log2(cube) * (-1.0 / 3.0))

        def tile_pass(vector, which, building):
            def slab(index, carry):
                at = pl.multiple_of(index * rows, rows)
                for t, part in pairs[which]:
                    if which == 0:
                        total_s = jnp.zeros((rows, atoms), jnp.float32)
                        total_t = jnp.zeros((rows, atoms), jnp.float32)
                    else:
                        total_s = sums[t, 0, pl.ds(at, rows), :]
                        total_t = sums[t, 1, pl.ds(at, rows), :]
                    if building:
                        own_part = [columns[t, f, pl.ds(at, rows), :] for f in range(4)]
                    for n, place in part:
                        x, y, z = place
                        if building:
                            block = coupling(t, n, place, at, own_part)
                            blocks[t, n, pl.ds(at, rows), :] = block
                            total_t = total_t - block
                        else:
                            block = blocks[t, n, pl.ds(at, rows), :]
                            total_t = total_t + block * vector[x, y, z, 1:2, :]
                        total_s = total_s + block * vector[x, y, z, 0:1, :]
                    sums[t, 0, pl.ds(at, rows), :] = total_s
                    sums[t, 1, pl.ds(at, rows), :] = total_t
                return carry

            lax.fori_loop(0, slabs, slab, 0)

        scale = 20.0 * COULOMB / CUTOFF
        ones = jnp.ones((16, 3 * atoms), jnp.bfloat16)

        def collect(vector, image):
            for t, (x, y, z) in enumerate(local):
                for s in range(2):
                    left = sums[t, s]
                    pieces = []
                    for k in range(3):
                        piece = left.astype(jnp.bfloat16)
                        pieces.append(piece)
                        if k < 2:
                            left = left - piece.astype(jnp.float32)
                    row = lax.dot_general(
                        ones,
                        jnp.concatenate(pieces, axis=1),
                        (((1,), (1,)), ((), ())),
                        preferred_element_type=jnp.float32,
                    )[0:1]
                    here = vector[x + 1, y + 1, z + 1, s : s + 1, :]
                    image(x, y, z, s, eta[t] * here + scale * row)

        def to_padded(buffer):
            def store(x, y, z, s, row):
                buffer[x + 1, y + 1, z + 1, s : s + 1, :] = row

            return store

        def to_own(x, y, z, s, row):
            own_image[x, y, z, s : s + 1, :] = row

        lane = lax.broadcasted_iota(jnp.int32, (2, atoms), 1)

        def over_own(values):
            return jnp.sum(jnp.sum(values, axis=(0, 1, 2)), axis=1, keepdims=True)

        def sum_copies(g, stage):
            axes, count = groups[g], group_sizes[g]
            return [
                pltpu.make_async_remote_copy(
                    src_ref=parts[g].at[stage, 0],
                    dst_ref=parts[g].at[stage, hop],
                    send_sem=sum_send.at[stage, g],
                    recv_sem=sum_recv.at[stage, g],
                    device_id=member(axes, hop),
                    device_id_type=MESH,
                )
                for hop in range(1, count)
            ]

        def whole_sum(g, stage):
            count = group_sizes[g]
            return pltpu.make_async_remote_copy(
                src_ref=parts[g].at[stage, pl.ds(1, count - 1)],
                dst_ref=parts[g].at[stage, pl.ds(1, count - 1)],
                send_sem=sum_send.at[stage, g],
                recv_sem=sum_recv.at[stage, g],
                device_id=member(groups[g], 1),
                device_id_type=MESH,
            )

        def start_sums(values, stage):
            message = jnp.zeros((2, atoms), jnp.float32)
            for k, value in enumerate(values):
                message = jnp.where(lane == k, value, message)
            parts[0][stage, 0] = message
            for copy in sum_copies(0, stage):
                copy.start()

        def finish_sums(number, stage):
            for g in range(len(groups)):
                whole_sum(g, stage).wait_recv()
                total = jnp.sum(parts[g][stage], axis=0)
                if g + 1 < len(groups):
                    parts[g + 1][stage, 0] = total
                    for copy in sum_copies(g + 1, stage):
                        copy.start()
            return [
                jnp.sum(jnp.where(lane == k, total, 0.0), axis=1, keepdims=True)
                for k in range(number)
            ]

        halo(fields, 0)
        with jax.named_scope("build0"):
            tile_pass(source, 0, True)
        for which in (1, 2):
            with jax.named_scope(f"wait_pos{which}"):
                arrived(fields, 0, which)
            locate([p for p in padded if reach(p) == which])
            with jax.named_scope(f"build{which}"):
                tile_pass(source, which, True)
        with jax.named_scope("collect0"):
            collect(source, to_padded(first))

        def apply(vector, stage):
            with jax.named_scope(f"pass{stage}_0"):
                tile_pass(vector, 0, False)
            for which in (1, 2):
                with jax.named_scope(f"wait{stage}_{which}"):
                    arrived(vector, stage, which)
                with jax.named_scope(f"pass{stage}_{which}"):
                    tile_pass(vector, which, False)
            with jax.named_scope(f"collect{stage}"):
                collect(vector, to_own)

        halo(first, 1)
        residual = source[own]
        image = first[own]
        start_sums([over_own(residual * residual), over_own(residual * image)], 0)
        apply(first, 1)
        with jax.named_scope("sums0"):
            norm_now, curvature = finish_sums(2, 0)
        step_size = norm_now / curvature
        direction, along = residual, image
        further = own_image[...]
        answer = step_size * direction
        residual = residual - step_size * along
        image = image - step_size * further
        second[own] = image
        halo(second, 2)
        start_sums([over_own(residual * residual), over_own(residual * image)], 1)
        apply(second, 2)
        with jax.named_scope("sums1"):
            norm_next, curvature = finish_sums(2, 1)
        growth = norm_next / norm_now
        step_size = norm_next / (curvature - growth * norm_next / step_size)
        norm_now = norm_next
        further = own_image[...] + growth * further
        direction = residual + growth * direction
        along = image + growth * along
        answer = answer + step_size * direction
        residual = residual - step_size * along
        image = image - step_size * further
        values = [residual * residual, residual * image, answer, residual, direction]
        start_sums([over_own(v) for v in values], 2)
        with jax.named_scope("sums2"):
            norm_next, curvature, *others = finish_sums(5, 2)
        growth = norm_next / norm_now
        step_size = norm_next / (curvature - growth * norm_next / step_size)
        answer = answer + step_size * (residual + growth * direction)
        residual = residual - step_size * (image + growth * along)
        totals = others[0] + step_size * (others[1] + growth * others[2])
        level = totals[0:1] / totals[1:2]
        for x, y, z in local:
            charge_ref[x, y, z : z + 1, :] = 1000.0 * (
                answer[x, y, z, 0:1] - level * answer[x, y, z, 1:2]
            )
            for s in range(2):
                resid_ref[s, x, y, z : z + 1, :] = residual[x, y, z, s : s + 1]
        with jax.named_scope("drain"):
            for stage, buffer in enumerate((fields, first, second)):
                for kind in range(KINDS):
                    whole_kind(buffer, stage, kind).wait_send()
            for stage in range(ITERS):
                for g in range(len(groups)):
                    whole_sum(g, stage).wait_send()

    scratch = [
        pltpu.VMEM((3,) + cells + (atoms,), jnp.float32),
        pltpu.VMEM(cells + (atoms,), jnp.int32),
        None,
        pltpu.SMEM((types,), jnp.float32),
        pltpu.SMEM((types,), jnp.float32),
        pltpu.SMEM((types,), jnp.float32),
        pltpu.VMEM(width + (4, atoms), jnp.float32),
        pltpu.VMEM(width + (4, atoms), jnp.float32),
        pltpu.VMEM((tiles, 4, atoms, atoms), jnp.float32),
        pltpu.VMEM((len(STEPS), tiles, atoms), jnp.float32),
        pltpu.VMEM((tiles, len(STEPS), atoms, atoms), jnp.float32),
        pltpu.VMEM((tiles, 2, atoms, atoms), jnp.float32),
        pltpu.VMEM(width + (2, atoms), jnp.float32),
        pltpu.VMEM(width + (2, atoms), jnp.float32),
        pltpu.VMEM(width + (2, atoms), jnp.float32),
        pltpu.VMEM(cells + (2, atoms), jnp.float32),
    ]
    scratch += [pltpu.VMEM((ITERS, count, 2, atoms), jnp.float32) for count in group_sizes]
    scratch += [
        pltpu.SemaphoreType.DMA((6,)),
        pltpu.SemaphoreType.DMA((ITERS, KINDS)),
        pltpu.SemaphoreType.DMA((ITERS, KINDS)),
        pltpu.SemaphoreType.DMA((ITERS, len(groups))),
        pltpu.SemaphoreType.DMA((ITERS, len(groups))),
    ]
    return kernel, scratch


def solution(mesh):
    sizes = {a: mesh.shape[a] for a in AXES}
    devices = sizes["gx"] * sizes["gy"] * sizes["gz"]
    groups = (AXES,) if devices <= 64 else tuple((a,) for a in AXES)

    def per_device(offsets, type_ids, neighbours, type_chi, type_eta, type_gamma):
        cells = offsets.shape[1:4]
        atoms = offsets.shape[4]
        types = type_chi.shape[0]
        kernel, scratch = make_kernel(sizes, groups, cells, atoms, types, 32)
        scratch[2] = pltpu.VMEM(neighbours.shape, jnp.int32)
        vmem = pl.BlockSpec(memory_space=pltpu.VMEM)
        hbm = pl.BlockSpec(memory_space=pltpu.HBM)
        return pl.pallas_call(
            kernel,
            out_shape=(
                jax.ShapeDtypeStruct(cells + (atoms,), jnp.float32),
                jax.ShapeDtypeStruct((2,) + cells + (atoms,), jnp.float32),
            ),
            in_specs=[hbm] * 6,
            out_specs=(vmem, vmem),
            scratch_shapes=scratch,
            compiler_params=pltpu.CompilerParams(
                collective_id=0, has_side_effects=True, vmem_limit_bytes=48 * 1024 * 1024
            ),
        )(offsets, type_ids, neighbours, type_chi, type_eta, type_gamma)

    placed = (
        P(None, "gx", "gy", "gz", None),
        P("gx", "gy", "gz", None),
        P("gx", "gy", "gz", None),
        P(),
        P(),
        P(),
    )
    return jax.shard_map(
        per_device,
        mesh=mesh,
        in_specs=placed,
        out_specs=(P("gx", "gy", "gz", None), P(None, "gx", "gy", "gz", None)),
        check_vma=False,
    )
```

```python
import itertools

import jax
import jax.numpy as jnp
from jax import lax
from jax.experimental import pallas as pl
from jax.experimental.pallas import tpu as pltpu
from jax.sharding import PartitionSpec as P

ITERS = 3
CELL_EDGE = 11.0
CUTOFF = 10.0
COULOMB = 14.4
AXES = ("gx", "gy", "gz")
FAR = 1000.0
MESH = pl.DeviceIdType.MESH
STEPS = [d for d in itertools.product((-1, 0, 1), repeat=3)]
REMOTE = sorted((d for d in STEPS if d != (0, 0, 0)), key=lambda d: (-abs(d[2]), -abs(d[0])))
KINDS = 3


def kind_of(step):
    return 2 if step[2] else (1 if step[0] else 0)


def rounded_sides(step, cells):
    source, target = [], []
    for d, c in zip(step, cells):
        if d == 0:
            source.append(pl.ds(1, c))
            target.append(pl.ds(1, c))
        elif d > 0:
            source.append(pl.ds(c, 1))
            target.append(pl.ds(0, 1))
        else:
            source.append(pl.ds(1, 1))
            target.append(pl.ds(c + 1, 1))
    return tuple(source), tuple(target)


def make_kernel(sizes, groups, cells, atoms, types, rows):
    width = tuple(c + 2 for c in cells)
    tiles = cells[0] * cells[1] * cells[2]
    local = list(itertools.product(*[range(c) for c in cells]))
    padded = list(itertools.product(*[range(w) for w in width]))
    own = tuple(slice(1, 1 + c) for c in cells)
    group_sizes = []
    for axes in groups:
        count = 1
        for a in axes:
            count = count * sizes[a]
        group_sizes.append(count)
    boxes = (
        (pl.ds(0, cells[0]), pl.ds(0, 2), pl.ds(0, cells[2])),
        (pl.ds(0, 2), pl.ds(0, width[1]), pl.ds(0, cells[2])),
        (pl.ds(0, width[0]), pl.ds(0, width[1]), pl.ds(0, 2)),
    )

    def linear(place):
        return (place[0] * width[1] + place[1]) * width[2] + place[2]

    def reach(place):
        if not 1 <= place[2] <= cells[2]:
            return 2
        return 0 if all(1 <= p <= c for p, c in zip(place, cells)) else 1

    pairs = [[], [], []]
    for t, home in enumerate(local):
        split = [[], [], []]
        for n, step in enumerate(STEPS):
            place = tuple(h + 1 + d for h, d in zip(home, step))
            split[reach(place)].append((n, place))
        for kept, part in zip(pairs, split):
            kept.append((t, part))

    def kernel(*refs):
        hbm, (charge_ref, resid_ref) = refs[:6], refs[6:8]
        (off_ref, type_ref, list_ref, chi_ref, eta_ref, gamma_ref) = refs[8:14]
        (fields, geometry, columns, listed, blocks, sums, source, first, second, own_image) = refs[14:24]
        parts = refs[24 : 24 + len(groups)]
        load_sem, halo_send, halo_recv, sum_send, sum_recv = refs[24 + len(groups) :]

        loads = [
            pltpu.make_async_copy(a, b, load_sem.at[k])
            for k, (a, b) in enumerate(
                zip(hbm, (off_ref, type_ref, list_ref, chi_ref, eta_ref, gamma_ref))
            )
        ]
        for load in loads:
            load.start()

        me = {a: lax.axis_index(a) for a in AXES}

        def neighbour(step):
            return tuple(
                lax.rem(me[a] + (d + sizes[a]), sizes[a]) for a, d in zip(AXES, step)
            )

        def member(axes, hop):
            rank = 0
            count = 1
            for a in axes:
                rank = rank * sizes[a] + me[a]
                count = count * sizes[a]
            rank = lax.rem(rank + hop, count)
            place = dict(me)
            for a in reversed(axes):
                place[a] = lax.rem(rank, sizes[a])
                rank = rank // sizes[a]
            return tuple(place[a] for a in AXES)

        def lookup(kinds, table):
            result = jnp.zeros(kinds.shape, jnp.float32)
            for k in range(types):
                result = jnp.where(kinds == float(k), table[k], result)
            return result

        barrier = pltpu.get_barrier_semaphore()
        greeted = 0
        for axes, count in zip(groups, group_sizes):
            for hop in range(1, count):
                pl.semaphore_signal(
                    barrier, inc=1, device_id=member(axes, hop), device_id_type=MESH
                )
                greeted += 1
        if len(groups) > 1:
            for step in REMOTE:
                pl.semaphore_signal(
                    barrier, inc=1, device_id=neighbour(step), device_id_type=MESH
                )
                greeted += 1

        for load in loads:
            load.wait()

        def tenth(values, f, place):
            return (values + CELL_EDGE * (place[f] - 1.0)) * (1.0 / CUTOFF)

        def sigma(kinds):
            root = lax.rsqrt(lookup(kinds, gamma_ref))
            return root * root * root * (CUTOFF**-1.5)

        for x, y, z in local:
            for f in range(3):
                fields[x + 1, y + 1, z + 1, f : f + 1, :] = off_ref[f, x, y, z : z + 1, :]
            fields[x + 1, y + 1, z + 1, 3:4, :] = type_ref[x, y, z : z + 1, :].astype(jnp.float32)

        def locate(places):
            for x, y, z in places:
                place = (x, y, z)
                kinds = fields[x, y, z, 3:4, :]
                for f in range(3):
                    geometry[x, y, z, f : f + 1, :] = tenth(fields[x, y, z, f : f + 1, :], f, place)
                geometry[x, y, z, 3:4, :] = sigma(kinds)
                source[x, y, z, 0:1, :] = -lookup(kinds, chi_ref)
                source[x, y, z, 1:2, :] = jnp.full((1, atoms), -1.0, jnp.float32)

        locate([p for p in padded if reach(p) == 0])
        for t, (x, y, z) in enumerate(local):
            for f in range(4):
                row = geometry[x + 1, y + 1, z + 1, f : f + 1, :]
                columns[t, f] = jnp.transpose(jnp.broadcast_to(row, (atoms, atoms)))
        entries = jnp.concatenate(
            [list_ref[x, y, z : z + 1, :] - linear((x + 1, y + 1, z + 1)) for x, y, z in local], 0
        )
        for n, step in enumerate(STEPS):
            found = jnp.max(
                jnp.where(entries == linear(step), 1.0, 0.0), axis=1, keepdims=True
            )
            listed[n] = jnp.broadcast_to(1.0 - (1.0 - found) * FAR, (tiles, atoms))
        eta = [lookup(fields[x + 1, y + 1, z + 1, 3:4, :], eta_ref) for x, y, z in local]

        with jax.named_scope("barrier"):
            pl.semaphore_wait(barrier, greeted)

        def halo(buffer, stage):
            for step in REMOTE:
                here, there = rounded_sides(step, cells)
                kind = kind_of(step)
                pltpu.make_async_remote_copy(
                    src_ref=buffer.at[here],
                    dst_ref=buffer.at[there],
                    send_sem=halo_send.at[stage, kind],
                    recv_sem=halo_recv.at[stage, kind],
                    device_id=neighbour(step),
                    device_id_type=MESH,
                ).start()

        def whole_kind(buffer, stage, kind):
            return pltpu.make_async_remote_copy(
                src_ref=buffer.at[boxes[kind]],
                dst_ref=buffer.at[boxes[kind]],
                send_sem=halo_send.at[stage, kind],
                recv_sem=halo_recv.at[stage, kind],
                device_id=neighbour(REMOTE[0]),
                device_id_type=MESH,
            )

        def arrived(buffer, stage, which):
            if which == 1:
                whole_kind(buffer, stage, 0).wait_recv()
                whole_kind(buffer, stage, 1).wait_recv()
            if which == 2:
                whole_kind(buffer, stage, 2).wait_recv()

        slabs = atoms // rows

        def coupling(t, n, place, at, own_part):
            near = [geometry[place[0], place[1], place[2], f : f + 1, :] for f in range(4)]
            dx = near[0] - own_part[0]
            dy = near[1] - own_part[1]
            dz = near[2] - own_part[2]
            square = dx * dx + dy * dy + dz * dz
            if STEPS[n] == (0, 0, 0):
                i = lax.broadcasted_iota(jnp.int32, (rows, atoms), 0) + at
                j = lax.broadcasted_iota(jnp.int32, (rows, atoms), 1)
                square = jnp.where(i == j, 4.0, square)
            u = square * lax.rsqrt(square)
            w = jnp.maximum(listed[n, t : t + 1, :] - u, 0.0)
            w = w * w
            w = w * w
            shape = (u + 0.5) * (square + 0.2) - 0.05
            cube = square * u + own_part[3] * near[3]
            return w * shape * jnp.exp2(jnp.log2(cube) * (-1.0 / 3.0))

        def tile_pass(vector, which, building):
            def slab(index, carry):
                at = pl.multiple_of(index * rows, rows)
                for t, part in pairs[which]:
                    if which == 0:
                        total_s = jnp.zeros((rows, atoms), jnp.float32)
                        total_t = jnp.zeros((rows, atoms), jnp.float32)
                    else:
                        total_s = sums[t, 0, pl.ds(at, rows), :]
                        total_t = sums[t, 1, pl.ds(at, rows), :]
                    if building:
                        own_part = [columns[t, f, pl.ds(at, rows), :] for f in range(4)]
                    for n, place in part:
                        x, y, z = place
                        if building:
                            block = coupling(t, n, place, at, own_part)
                            blocks[t, n, pl.ds(at, rows), :] = block
                            total_t = total_t - block
                        else:
                            block = blocks[t, n, pl.ds(at, rows), :]
                            total_t = total_t + block * vector[x, y, z, 1:2, :]
                        total_s = total_s + block * vector[x, y, z, 0:1, :]
                    sums[t, 0, pl.ds(at, rows), :] = total_s
                    sums[t, 1, pl.ds(at, rows), :] = total_t
                return carry

            lax.fori_loop(0, slabs, slab, 0)

        scale = 20.0 * COULOMB / CUTOFF
        ones = jnp.ones((16, 3 * atoms), jnp.bfloat16)

        def collect(vector, image):
            for t, (x, y, z) in enumerate(local):
                for s in range(2):
                    left = sums[t, s]
                    pieces = []
                    for k in range(3):
                        piece = left.astype(jnp.bfloat16)
                        pieces.append(piece)
                        if k < 2:
                            left = left - piece.astype(jnp.float32)
                    row = lax.dot_general(
                        ones,
                        jnp.concatenate(pieces, axis=1),
                        (((1,), (1,)), ((), ())),
                        preferred_element_type=jnp.float32,
                    )[0:1]
                    here = vector[x + 1, y + 1, z + 1, s : s + 1, :]
                    image(x, y, z, s, eta[t] * here + scale * row)

        def to_padded(buffer):
            def store(x, y, z, s, row):
                buffer[x + 1, y + 1, z + 1, s : s + 1, :] = row

            return store

        def to_own(x, y, z, s, row):
            own_image[x, y, z, s : s + 1, :] = row

        lane = lax.broadcasted_iota(jnp.int32, (2, atoms), 1)

        def over_own(values):
            return jnp.sum(jnp.sum(values, axis=(0, 1, 2)), axis=1, keepdims=True)

        def sum_copies(g, stage):
            axes, count = groups[g], group_sizes[g]
            return [
                pltpu.make_async_remote_copy(
                    src_ref=parts[g].at[stage, 0],
                    dst_ref=parts[g].at[stage, hop],
                    send_sem=sum_send.at[stage, g],
                    recv_sem=sum_recv.at[stage, g],
                    device_id=member(axes, hop),
                    device_id_type=MESH,
                )
                for hop in range(1, count)
            ]

        def whole_sum(g, stage):
            count = group_sizes[g]
            return pltpu.make_async_remote_copy(
                src_ref=parts[g].at[stage, pl.ds(1, count - 1)],
                dst_ref=parts[g].at[stage, pl.ds(1, count - 1)],
                send_sem=sum_send.at[stage, g],
                recv_sem=sum_recv.at[stage, g],
                device_id=member(groups[g], 1),
                device_id_type=MESH,
            )

        def start_sums(values, stage):
            message = jnp.zeros((2, atoms), jnp.float32)
            for k, value in enumerate(values):
                message = jnp.where(lane == k, value, message)
            parts[0][stage, 0] = message
            for copy in sum_copies(0, stage):
                copy.start()

        def finish_sums(number, stage):
            for g in range(len(groups)):
                whole_sum(g, stage).wait_recv()
                total = jnp.sum(parts[g][stage], axis=0)
                if g + 1 < len(groups):
                    parts[g + 1][stage, 0] = total
                    for copy in sum_copies(g + 1, stage):
                        copy.start()
            return [
                jnp.sum(jnp.where(lane == k, total, 0.0), axis=1, keepdims=True)
                for k in range(number)
            ]

        halo(fields, 0)
        with jax.named_scope("build0"):
            tile_pass(source, 0, True)
        for which in (1, 2):
            with jax.named_scope(f"wait_pos{which}"):
                arrived(fields, 0, which)
            locate([p for p in padded if reach(p) == which])
            with jax.named_scope(f"build{which}"):
                tile_pass(source, which, True)
        with jax.named_scope("collect0"):
            collect(source, to_padded(first))

        def apply(vector, stage):
            with jax.named_scope(f"pass{stage}_0"):
                tile_pass(vector, 0, False)
            for which in (1, 2):
                with jax.named_scope(f"wait{stage}_{which}"):
                    arrived(vector, stage, which)
                with jax.named_scope(f"pass{stage}_{which}"):
                    tile_pass(vector, which, False)
            with jax.named_scope(f"collect{stage}"):
                collect(vector, to_own)

        halo(first, 1)
        residual = source[own]
        image = first[own]
        start_sums([over_own(residual * residual), over_own(residual * image)], 0)
        apply(first, 1)
        with jax.named_scope("sums0"):
            norm_now, curvature = finish_sums(2, 0)
        step_size = norm_now / curvature
        direction, along = residual, image
        further = own_image[...]
        answer = step_size * direction
        residual = residual - step_size * along
        image = image - step_size * further
        second[own] = image
        halo(second, 2)
        start_sums([over_own(residual * residual), over_own(residual * image)], 1)
        apply(second, 2)
        with jax.named_scope("sums1"):
            norm_next, curvature = finish_sums(2, 1)
        growth = norm_next / norm_now
        step_size = norm_next / (curvature - growth * norm_next / step_size)
        norm_now = norm_next
        further = own_image[...] + growth * further
        direction = residual + growth * direction
        along = image + growth * along
        answer = answer + step_size * direction
        residual = residual - step_size * along
        image = image - step_size * further
        values = [residual * residual, residual * image, answer, residual, direction]
        start_sums([over_own(v) for v in values], 2)
        with jax.named_scope("sums2"):
            norm_next, curvature, *others = finish_sums(5, 2)
        growth = norm_next / norm_now
        step_size = norm_next / (curvature - growth * norm_next / step_size)
        answer = answer + step_size * (residual + growth * direction)
        residual = residual - step_size * (image + growth * along)
        totals = others[0] + step_size * (others[1] + growth * others[2])
        level = totals[0:1] / totals[1:2]
        for x, y, z in local:
            charge_ref[x, y, z : z + 1, :] = 1000.0 * (
                answer[x, y, z, 0:1] - level * answer[x, y, z, 1:2]
            )
            for s in range(2):
                resid_ref[s, x, y, z : z + 1, :] = residual[x, y, z, s : s + 1]
        with jax.named_scope("drain"):
            for stage, buffer in enumerate((fields, first, second)):
                for kind in range(KINDS):
                    whole_kind(buffer, stage, kind).wait_send()
            for stage in range(ITERS):
                for g in range(len(groups)):
                    whole_sum(g, stage).wait_send()

    scratch = [
        pltpu.VMEM((3,) + cells + (atoms,), jnp.float32),
        pltpu.VMEM(cells + (atoms,), jnp.int32),
        None,
        pltpu.SMEM((types,), jnp.float32),
        pltpu.SMEM((types,), jnp.float32),
        pltpu.SMEM((types,), jnp.float32),
        pltpu.VMEM(width + (4, atoms), jnp.float32),
        pltpu.VMEM(width + (4, atoms), jnp.float32),
        pltpu.VMEM((tiles, 4, atoms, atoms), jnp.float32),
        pltpu.VMEM((len(STEPS), tiles, atoms), jnp.float32),
        pltpu.VMEM((tiles, len(STEPS), atoms, atoms), jnp.float32),
        pltpu.VMEM((tiles, 2, atoms, atoms), jnp.float32),
        pltpu.VMEM(width + (2, atoms), jnp.float32),
        pltpu.VMEM(width + (2, atoms), jnp.float32),
        pltpu.VMEM(width + (2, atoms), jnp.float32),
        pltpu.VMEM(cells + (2, atoms), jnp.float32),
    ]
    scratch += [pltpu.VMEM((ITERS, count, 2, atoms), jnp.float32) for count in group_sizes]
    scratch += [
        pltpu.SemaphoreType.DMA((6,)),
        pltpu.SemaphoreType.DMA((ITERS, KINDS)),
        pltpu.SemaphoreType.DMA((ITERS, KINDS)),
        pltpu.SemaphoreType.DMA((ITERS, len(groups))),
        pltpu.SemaphoreType.DMA((ITERS, len(groups))),
    ]
    return kernel, scratch


def solution(mesh):
    sizes = {a: mesh.shape[a] for a in AXES}
    devices = sizes["gx"] * sizes["gy"] * sizes["gz"]
    groups = (AXES,) if devices <= 64 else tuple((a,) for a in AXES)

    def per_device(offsets, type_ids, neighbours, type_chi, type_eta, type_gamma):
        cells = offsets.shape[1:4]
        atoms = offsets.shape[4]
        types = type_chi.shape[0]
        kernel, scratch = make_kernel(sizes, groups, cells, atoms, types, 32)
        scratch[2] = pltpu.VMEM(neighbours.shape, jnp.int32)
        vmem = pl.BlockSpec(memory_space=pltpu.VMEM)
        hbm = pl.BlockSpec(memory_space=pltpu.HBM)
        return pl.pallas_call(
            kernel,
            out_shape=(
                jax.ShapeDtypeStruct(cells + (atoms,), jnp.float32),
                jax.ShapeDtypeStruct((2,) + cells + (atoms,), jnp.float32),
            ),
            in_specs=[hbm] * 6,
            out_specs=(vmem, vmem),
            scratch_shapes=scratch,
            compiler_params=pltpu.CompilerParams(
                collective_id=0, has_side_effects=True, vmem_limit_bytes=48 * 1024 * 1024
            ),
        )(*[pltpu.with_memory_space_constraint(v, pltpu.HBM) for v in (offsets, type_ids, neighbours, type_chi, type_eta, type_gamma)])

    placed = (
        P(None, "gx", "gy", "gz", None),
        P("gx", "gy", "gz", None),
        P("gx", "gy", "gz", None),
        P(),
        P(),
        P(),
    )
    return jax.shard_map(
        per_device,
        mesh=mesh,
        in_specs=placed,
        out_specs=(P("gx", "gy", "gz", None), P(None, "gx", "gy", "gz", None)),
        check_vma=False,
    )
```

```python
import itertools

import jax
import jax.numpy as jnp
from jax import lax
from jax.experimental import pallas as pl
from jax.experimental.pallas import tpu as pltpu
from jax.sharding import PartitionSpec as P

ITERS = 3
CELL_EDGE = 11.0
CUTOFF = 10.0
COULOMB = 14.4
AXES = ("gx", "gy", "gz")
FAR = 1000.0
MESH = pl.DeviceIdType.MESH
STEPS = [d for d in itertools.product((-1, 0, 1), repeat=3)]
REMOTE = sorted((d for d in STEPS if d != (0, 0, 0)), key=lambda d: (-abs(d[2]), -abs(d[0])))
KINDS = 3


def kind_of(step):
    return 2 if step[2] else (1 if step[0] else 0)


def rounded_sides(step, cells):
    source, target = [], []
    for d, c in zip(step, cells):
        if d == 0:
            source.append(pl.ds(1, c))
            target.append(pl.ds(1, c))
        elif d > 0:
            source.append(pl.ds(c, 1))
            target.append(pl.ds(0, 1))
        else:
            source.append(pl.ds(1, 1))
            target.append(pl.ds(c + 1, 1))
    return tuple(source), tuple(target)


def make_kernel(sizes, groups, cells, atoms, types, rows):
    width = tuple(c + 2 for c in cells)
    tiles = cells[0] * cells[1] * cells[2]
    local = list(itertools.product(*[range(c) for c in cells]))
    padded = list(itertools.product(*[range(w) for w in width]))
    own = tuple(slice(1, 1 + c) for c in cells)
    group_sizes = []
    for axes in groups:
        count = 1
        for a in axes:
            count = count * sizes[a]
        group_sizes.append(count)
    boxes = (
        (pl.ds(0, cells[0]), pl.ds(0, 2), pl.ds(0, cells[2])),
        (pl.ds(0, 2), pl.ds(0, width[1]), pl.ds(0, cells[2])),
        (pl.ds(0, width[0]), pl.ds(0, width[1]), pl.ds(0, 2)),
    )

    def linear(place):
        return (place[0] * width[1] + place[1]) * width[2] + place[2]

    def reach(place):
        if not 1 <= place[2] <= cells[2]:
            return 2
        return 0 if all(1 <= p <= c for p, c in zip(place, cells)) else 1

    pairs = [[], [], []]
    for t, home in enumerate(local):
        split = [[], [], []]
        for n, step in enumerate(STEPS):
            place = tuple(h + 1 + d for h, d in zip(home, step))
            split[reach(place)].append((n, place))
        for kept, part in zip(pairs, split):
            kept.append((t, part))

    def kernel(*refs):
        hbm, (charge_ref, resid_ref) = refs[:6], refs[6:8]
        (off_ref, type_ref, list_ref, chi_ref, eta_ref, gamma_ref) = refs[8:14]
        (fields, geometry, shields, columns, listed, blocks, sums, source) = refs[14:22]
        (first, second, own_image) = refs[22:25]
        parts = refs[25 : 25 + len(groups)]
        load_sem, halo_send, halo_recv, sum_send, sum_recv = refs[25 + len(groups) :]

        loads = [
            pltpu.make_async_copy(a, b, load_sem.at[k])
            for k, (a, b) in enumerate(
                zip(hbm, (off_ref, type_ref, list_ref, chi_ref, eta_ref, gamma_ref))
            )
        ]
        me = {a: lax.axis_index(a) for a in AXES}

        def neighbour(step):
            return tuple(
                lax.rem(me[a] + (d + sizes[a]), sizes[a]) for a, d in zip(AXES, step)
            )

        def member(axes, hop):
            rank = 0
            count = 1
            for a in axes:
                rank = rank * sizes[a] + me[a]
                count = count * sizes[a]
            rank = lax.rem(rank + hop, count)
            place = dict(me)
            for a in reversed(axes):
                place[a] = lax.rem(rank, sizes[a])
                rank = rank // sizes[a]
            return tuple(place[a] for a in AXES)

        def lookup(kinds, table):
            result = jnp.zeros(kinds.shape, jnp.float32)
            for k in range(types):
                result = jnp.where(kinds == float(k), table[k], result)
            return result

        for load in loads[:2]:
            load.start()
        barrier = pltpu.get_barrier_semaphore()
        greeted = 0
        for axes, count in zip(groups, group_sizes):
            for hop in range(1, count):
                pl.semaphore_signal(
                    barrier, inc=1, device_id=member(axes, hop), device_id_type=MESH
                )
                greeted += 1
        if len(groups) > 1:
            for step in REMOTE:
                pl.semaphore_signal(
                    barrier, inc=1, device_id=neighbour(step), device_id_type=MESH
                )
                greeted += 1

        for load in loads[2:]:
            load.start()
        for load in loads[:2]:
            load.wait()

        row4 = lax.broadcasted_iota(jnp.int32, (4, atoms), 0)

        def shifted(place):
            parts = [CELL_EDGE * (p - 1.0 - 0.5 * c) for p, c in zip(place, cells)]
            return jnp.where(row4 == 0, parts[0], jnp.where(row4 == 1, parts[1], parts[2]))

        def stacked(raw, place):
            p = jnp.where(row4 < 3, (raw + shifted(place)) * (1.0 / CUTOFF), 0.0)
            return jnp.where(row4 < 3, p, jnp.sum(p * p, axis=0, keepdims=True))

        def thirds(values):
            pieces = []
            for k in range(3):
                piece = values.astype(jnp.bfloat16).astype(jnp.float32)
                pieces.append(piece)
                if k < 2:
                    values = values - piece
            return pieces

        def sigma(kinds):
            root = lax.rsqrt(lookup(kinds, gamma_ref))
            return root * root * root * (CUTOFF**-1.5)

        for x, y, z in local:
            for f in range(3):
                fields[x + 1, y + 1, z + 1, f : f + 1, :] = off_ref[f, x, y, z : z + 1, :]
            fields[x + 1, y + 1, z + 1, 3:4, :] = type_ref[x, y, z : z + 1, :].astype(jnp.float32)

        def locate(places):
            for x, y, z in places:
                place = (x, y, z)
                kinds = fields[x, y, z, 3:4, :]
                v1, v2, v3 = thirds(stacked(fields[x, y, z], place))
                unit = jnp.where(row4 < 3, 1.0, 0.0)
                geometry[x, y, z] = jnp.concatenate(
                    [v1, v2, v3, v1, v2, v1, unit, jnp.zeros_like(unit)], axis=0
                )
                shields[x, y, z, 0:1, :] = sigma(kinds)
                source[x, y, z, 0:1, :] = -lookup(kinds, chi_ref)
                source[x, y, z, 1:2, :] = jnp.full((1, atoms), -1.0, jnp.float32)

        with jax.named_scope("barrier"):
            pl.semaphore_wait(barrier, greeted)

        def halo(buffer, stage):
            for step in REMOTE:
                here, there = rounded_sides(step, cells)
                kind = kind_of(step)
                pltpu.make_async_remote_copy(
                    src_ref=buffer.at[here],
                    dst_ref=buffer.at[there],
                    send_sem=halo_send.at[stage, kind],
                    recv_sem=halo_recv.at[stage, kind],
                    device_id=neighbour(step),
                    device_id_type=MESH,
                ).start()

        def whole_kind(buffer, stage, kind):
            return pltpu.make_async_remote_copy(
                src_ref=buffer.at[boxes[kind]],
                dst_ref=buffer.at[boxes[kind]],
                send_sem=halo_send.at[stage, kind],
                recv_sem=halo_recv.at[stage, kind],
                device_id=neighbour(REMOTE[0]),
                device_id_type=MESH,
            )

        def arrived(buffer, stage, which):
            if which == 1:
                whole_kind(buffer, stage, 0).wait_recv()
                whole_kind(buffer, stage, 1).wait_recv()
            if which == 2:
                whole_kind(buffer, stage, 2).wait_recv()

        slabs = atoms // rows

        def coupling(t, n, place, at, own_part):
            square = lax.dot_general(
                own_part[0][:, :32],
                geometry[place],
                (((1,), (0,)), ((), ())),
                preferred_element_type=jnp.float32,
            )
            if STEPS[n] == (0, 0, 0):
                i = lax.broadcasted_iota(jnp.int32, (rows, atoms), 0) + at
                j = lax.broadcasted_iota(jnp.int32, (rows, atoms), 1)
                square = jnp.where(i == j, 4.0, square)
            u = square * lax.rsqrt(square)
            w = jnp.maximum(listed[n, t : t + 1, :] - u, 0.0)
            w = w * w
            w = w * w
            shape = (u + 0.5) * (square + 0.2) - 0.05
            cube = square * u + own_part[1] * shields[place[0], place[1], place[2], 0:1, :]
            return w * shape * jnp.exp2(jnp.log2(cube) * (-1.0 / 3.0))

        def tile_pass(vector, which, building):
            def slab(index, carry):
                at = pl.multiple_of(index * rows, rows)
                for t, part in pairs[which]:
                    if which == 0:
                        total_s = jnp.zeros((rows, atoms), jnp.float32)
                        total_t = jnp.zeros((rows, atoms), jnp.float32)
                    else:
                        total_s = sums[t, 0, pl.ds(at, rows), :]
                        total_t = sums[t, 1, pl.ds(at, rows), :]
                    if building:
                        own_part = [columns[t, f, pl.ds(at, rows), :] for f in range(2)]
                    for n, place in part:
                        x, y, z = place
                        if building:
                            block = coupling(t, n, place, at, own_part)
                            blocks[t, n, pl.ds(at, rows), :] = block
                            total_t = total_t - block
                        else:
                            block = blocks[t, n, pl.ds(at, rows), :]
                            total_t = total_t + block * vector[x, y, z, 1:2, :]
                        total_s = total_s + block * vector[x, y, z, 0:1, :]
                    sums[t, 0, pl.ds(at, rows), :] = total_s
                    sums[t, 1, pl.ds(at, rows), :] = total_t
                return carry

            lax.fori_loop(0, slabs, slab, 0)

        scale = 20.0 * COULOMB / CUTOFF
        ones = jnp.ones((16, 3 * atoms), jnp.bfloat16)

        def collect(vector, image):
            for t, (x, y, z) in enumerate(local):
                for s in range(2):
                    left = sums[t, s]
                    pieces = []
                    for k in range(3):
                        piece = left.astype(jnp.bfloat16)
                        pieces.append(piece)
                        if k < 2:
                            left = left - piece.astype(jnp.float32)
                    row = lax.dot_general(
                        ones,
                        jnp.concatenate(pieces, axis=1),
                        (((1,), (1,)), ((), ())),
                        preferred_element_type=jnp.float32,
                    )[0:1]
                    here = vector[x + 1, y + 1, z + 1, s : s + 1, :]
                    image(x, y, z, s, eta[t] * here + scale * row)

        def to_padded(buffer):
            def store(x, y, z, s, row):
                buffer[x + 1, y + 1, z + 1, s : s + 1, :] = row

            return store

        def to_own(x, y, z, s, row):
            own_image[x, y, z, s : s + 1, :] = row

        lane = lax.broadcasted_iota(jnp.int32, (2, atoms), 1)

        def over_own(values):
            return jnp.sum(jnp.sum(values, axis=(0, 1, 2)), axis=1, keepdims=True)

        def sum_copies(g, stage):
            axes, count = groups[g], group_sizes[g]
            return [
                pltpu.make_async_remote_copy(
                    src_ref=parts[g].at[stage, 0],
                    dst_ref=parts[g].at[stage, hop],
                    send_sem=sum_send.at[stage, g],
                    recv_sem=sum_recv.at[stage, g],
                    device_id=member(axes, hop),
                    device_id_type=MESH,
                )
                for hop in range(1, count)
            ]

        def whole_sum(g, stage):
            count = group_sizes[g]
            return pltpu.make_async_remote_copy(
                src_ref=parts[g].at[stage, pl.ds(1, count - 1)],
                dst_ref=parts[g].at[stage, pl.ds(1, count - 1)],
                send_sem=sum_send.at[stage, g],
                recv_sem=sum_recv.at[stage, g],
                device_id=member(groups[g], 1),
                device_id_type=MESH,
            )

        def start_sums(values, stage):
            message = jnp.zeros((2, atoms), jnp.float32)
            for k, value in enumerate(values):
                message = jnp.where(lane == k, value, message)
            parts[0][stage, 0] = message
            for copy in sum_copies(0, stage):
                copy.start()

        def finish_sums(number, stage):
            for g in range(len(groups)):
                whole_sum(g, stage).wait_recv()
                total = jnp.sum(parts[g][stage], axis=0)
                if g + 1 < len(groups):
                    parts[g + 1][stage, 0] = total
                    for copy in sum_copies(g + 1, stage):
                        copy.start()
            return [
                jnp.sum(jnp.where(lane == k, total, 0.0), axis=1, keepdims=True)
                for k in range(number)
            ]

        halo(fields, 0)
        for load in loads[2:]:
            load.wait()
        locate([p for p in padded if reach(p) == 0])
        for t, (x, y, z) in enumerate(local):
            place = (x + 1, y + 1, z + 1)
            v1, v2, v3 = thirds(stacked(fields[place], place))
            c1 = jnp.where(row4 < 3, -2.0 * v1, 1.0)
            c2 = jnp.where(row4 < 3, -2.0 * v2, 0.0)
            c3 = jnp.where(row4 < 3, -2.0 * v3, 0.0)
            norms = jnp.where(
                row4 == 0, v1[3:4], jnp.where(row4 == 1, v2[3:4], jnp.where(row4 == 2, v3[3:4], 0.0))
            )
            none = jnp.zeros((atoms - 28, atoms), jnp.float32)
            columns[t, 0] = jnp.transpose(
                jnp.concatenate([c1, c1, c1, c2, c2, c3, norms, none], axis=0)
            )
            row = shields[x + 1, y + 1, z + 1, 0:1, :]
            columns[t, 1] = jnp.transpose(jnp.broadcast_to(row, (atoms, atoms)))
        entries = jnp.concatenate(
            [list_ref[x, y, z : z + 1, :] - linear((x + 1, y + 1, z + 1)) for x, y, z in local], 0
        )
        for n, step in enumerate(STEPS):
            found = jnp.max(
                jnp.where(entries == linear(step), 1.0, 0.0), axis=1, keepdims=True
            )
            listed[n] = jnp.broadcast_to(1.0 - (1.0 - found) * FAR, (tiles, atoms))
        eta = [lookup(fields[x + 1, y + 1, z + 1, 3:4, :], eta_ref) for x, y, z in local]

        with jax.named_scope("build0"):
            tile_pass(source, 0, True)
        for which in (1, 2):
            with jax.named_scope(f"wait_pos{which}"):
                arrived(fields, 0, which)
            locate([p for p in padded if reach(p) == which])
            with jax.named_scope(f"build{which}"):
                tile_pass(source, which, True)
        with jax.named_scope("collect0"):
            collect(source, to_padded(first))

        def apply(vector, stage):
            with jax.named_scope(f"pass{stage}_0"):
                tile_pass(vector, 0, False)
            for which in (1, 2):
                with jax.named_scope(f"wait{stage}_{which}"):
                    arrived(vector, stage, which)
                with jax.named_scope(f"pass{stage}_{which}"):
                    tile_pass(vector, which, False)
            with jax.named_scope(f"collect{stage}"):
                collect(vector, to_own)

        halo(first, 1)
        residual = source[own]
        image = first[own]
        start_sums([over_own(residual * residual), over_own(residual * image)], 0)
        apply(first, 1)
        with jax.named_scope("sums0"):
            norm_now, curvature = finish_sums(2, 0)
        step_size = norm_now / curvature
        direction, along = residual, image
        further = own_image[...]
        answer = step_size * direction
        residual = residual - step_size * along
        image = image - step_size * further
        second[own] = image
        halo(second, 2)
        start_sums([over_own(residual * residual), over_own(residual * image)], 1)
        apply(second, 2)
        with jax.named_scope("sums1"):
            norm_next, curvature = finish_sums(2, 1)
        growth = norm_next / norm_now
        step_size = norm_next / (curvature - growth * norm_next / step_size)
        norm_now = norm_next
        further = own_image[...] + growth * further
        direction = residual + growth * direction
        along = image + growth * along
        answer = answer + step_size * direction
        residual = residual - step_size * along
        image = image - step_size * further
        values = [residual * residual, residual * image, answer, residual, direction]
        start_sums([over_own(v) for v in values], 2)
        with jax.named_scope("sums2"):
            norm_next, curvature, *others = finish_sums(5, 2)
        growth = norm_next / norm_now
        step_size = norm_next / (curvature - growth * norm_next / step_size)
        answer = answer + step_size * (residual + growth * direction)
        residual = residual - step_size * (image + growth * along)
        totals = others[0] + step_size * (others[1] + growth * others[2])
        level = totals[0:1] / totals[1:2]
        for x, y, z in local:
            charge_ref[x, y, z : z + 1, :] = 1000.0 * (
                answer[x, y, z, 0:1] - level * answer[x, y, z, 1:2]
            )
            for s in range(2):
                resid_ref[s, x, y, z : z + 1, :] = residual[x, y, z, s : s + 1]
        with jax.named_scope("drain"):
            for stage, buffer in enumerate((fields, first, second)):
                for kind in range(KINDS):
                    whole_kind(buffer, stage, kind).wait_send()
            for stage in range(ITERS):
                for g in range(len(groups)):
                    whole_sum(g, stage).wait_send()

    scratch = [
        pltpu.VMEM((3,) + cells + (atoms,), jnp.float32),
        pltpu.VMEM(cells + (atoms,), jnp.int32),
        None,
        pltpu.SMEM((types,), jnp.float32),
        pltpu.SMEM((types,), jnp.float32),
        pltpu.SMEM((types,), jnp.float32),
        pltpu.VMEM(width + (4, atoms), jnp.float32),
        pltpu.VMEM(width + (32, atoms), jnp.float32),
        pltpu.VMEM(width + (1, atoms), jnp.float32),
        pltpu.VMEM((tiles, 2, atoms, atoms), jnp.float32),
        pltpu.VMEM((len(STEPS), tiles, atoms), jnp.float32),
        pltpu.VMEM((tiles, len(STEPS), atoms, atoms), jnp.float32),
        pltpu.VMEM((tiles, 2, atoms, atoms), jnp.float32),
        pltpu.VMEM(width + (2, atoms), jnp.float32),
        pltpu.VMEM(width + (2, atoms), jnp.float32),
        pltpu.VMEM(width + (2, atoms), jnp.float32),
        pltpu.VMEM(cells + (2, atoms), jnp.float32),
    ]
    scratch += [pltpu.VMEM((ITERS, count, 2, atoms), jnp.float32) for count in group_sizes]
    scratch += [
        pltpu.SemaphoreType.DMA((6,)),
        pltpu.SemaphoreType.DMA((ITERS, KINDS)),
        pltpu.SemaphoreType.DMA((ITERS, KINDS)),
        pltpu.SemaphoreType.DMA((ITERS, len(groups))),
        pltpu.SemaphoreType.DMA((ITERS, len(groups))),
    ]
    return kernel, scratch


def put_out(charge_in, resid_in, charge_ref, resid_ref, sems):
    copies = [
        pltpu.make_async_copy(charge_in, charge_ref, sems.at[0]),
        pltpu.make_async_copy(resid_in, resid_ref, sems.at[1]),
    ]
    for copy in copies:
        copy.start()
    for copy in copies:
        copy.wait()


def solution(mesh):
    sizes = {a: mesh.shape[a] for a in AXES}
    devices = sizes["gx"] * sizes["gy"] * sizes["gz"]
    groups = (AXES,) if devices <= 64 else tuple((a,) for a in AXES)

    def per_device(offsets, type_ids, neighbours, type_chi, type_eta, type_gamma):
        cells = offsets.shape[1:4]
        atoms = offsets.shape[4]
        types = type_chi.shape[0]
        kernel, scratch = make_kernel(sizes, groups, cells, atoms, types, 128)
        scratch[2] = pltpu.VMEM(neighbours.shape, jnp.int32)
        vmem = pl.BlockSpec(memory_space=pltpu.VMEM)
        hbm = pl.BlockSpec(memory_space=pltpu.HBM)
        pair = pl.pallas_call(
            kernel,
            out_shape=(
                jax.ShapeDtypeStruct(cells + (atoms,), jnp.float32),
                jax.ShapeDtypeStruct((2,) + cells + (atoms,), jnp.float32),
            ),
            in_specs=[hbm] * 6,
            out_specs=(vmem, vmem),
            scratch_shapes=scratch,
            compiler_params=pltpu.CompilerParams(
                collective_id=0, has_side_effects=True, vmem_limit_bytes=48 * 1024 * 1024
            ),
        )(*[pltpu.with_memory_space_constraint(v, pltpu.HBM) for v in (offsets, type_ids, neighbours, type_chi, type_eta, type_gamma)])
        return pl.pallas_call(
            put_out,
            out_shape=tuple(jax.ShapeDtypeStruct(v.shape, v.dtype) for v in pair),
            in_specs=[vmem] * 2,
            out_specs=(hbm, hbm),
            scratch_shapes=[pltpu.SemaphoreType.DMA((2,))],
        )(*[pltpu.with_memory_space_constraint(v, pltpu.VMEM) for v in pair])

    placed = (
        P(None, "gx", "gy", "gz", None),
        P("gx", "gy", "gz", None),
        P("gx", "gy", "gz", None),
        P(),
        P(),
        P(),
    )
    return jax.shard_map(
        per_device,
        mesh=mesh,
        in_specs=placed,
        out_specs=(P("gx", "gy", "gz", None), P(None, "gx", "gy", "gz", None)),
        check_vma=False,
    )
```

```python
import itertools

import jax
import jax.numpy as jnp
from jax import lax
from jax.experimental import pallas as pl
from jax.experimental.pallas import tpu as pltpu
from jax.sharding import PartitionSpec as P

ITERS = 3
CELL_EDGE = 11.0
CUTOFF = 10.0
COULOMB = 14.4
AXES = ("gx", "gy", "gz")
FAR = 1000.0
MESH = pl.DeviceIdType.MESH
STEPS = [d for d in itertools.product((-1, 0, 1), repeat=3)]
REMOTE = sorted((d for d in STEPS if d != (0, 0, 0)), key=lambda d: (-abs(d[2]), -abs(d[0])))
DISTANT = [d for d in REMOTE if d[2]]
CLOSE = [d for d in REMOTE if not d[2]]
KINDS = 6


def rounded_sides(step, cells):
    source, target = [], []
    for d, c in zip(step, cells):
        if d == 0:
            source.append(pl.ds(1, c))
            target.append(pl.ds(1, c))
        elif d > 0:
            source.append(pl.ds(c, 1))
            target.append(pl.ds(0, 1))
        else:
            source.append(pl.ds(1, 1))
            target.append(pl.ds(c + 1, 1))
    return tuple(source), tuple(target)


def make_kernel(sizes, groups, cells, atoms, types, rows):
    width = tuple(c + 2 for c in cells)
    tiles = cells[0] * cells[1] * cells[2]
    local = list(itertools.product(*[range(c) for c in cells]))
    padded = list(itertools.product(*[range(w) for w in width]))
    own = tuple(slice(1, 1 + c) for c in cells)
    group_sizes = []
    for axes in groups:
        count = 1
        for a in axes:
            count = count * sizes[a]
        group_sizes.append(count)
    boxes = (
        (pl.ds(0, cells[0]), pl.ds(0, 2), pl.ds(0, cells[2])),
        (pl.ds(0, 2), pl.ds(0, 2), pl.ds(0, cells[2])),
        (pl.ds(0, width[0]), pl.ds(0, width[1]), pl.ds(0, 1)),
        (pl.ds(0, 1), pl.ds(0, cells[1]), pl.ds(0, cells[2])),
        (pl.ds(0, 1), pl.ds(0, cells[1]), pl.ds(0, cells[2])),
        (pl.ds(0, width[0]), pl.ds(0, width[1]), pl.ds(0, 1)),
    )
    paired = cells[0] == 1 and sizes["gx"] % 2 == 0
    planes = paired and len(groups) == 1
    base = atoms // (2 * tiles)

    def linear(place):
        return (place[0] * width[1] + place[1]) * width[2] + place[2]

    def inside(place, axes):
        return all(1 <= place[a] <= cells[a] for a in axes)

    def reach(place):
        if inside(place, (0, 1, 2)):
            return 0
        if not inside(place, (2,)):
            return 3
        return 1 if paired and inside(place, (1,)) and place[0] == 0 else 2

    def kernel(*refs):
        hbm, (charge_ref, resid_ref) = refs[:6], refs[6:8]
        (off_ref, type_ref, list_ref, chi_ref, eta_ref, gamma_ref) = refs[8:14]
        (fields, geometry, shields, columns, listed, blocks, sums, source) = refs[14:22]
        (first, second, own_image) = refs[22:25]
        parts = refs[25 : 25 + len(groups)]
        load_sem, halo_send, halo_recv, sum_send, sum_recv, met = refs[25 + len(groups) :]

        loads = [
            pltpu.make_async_copy(a, b, load_sem.at[k])
            for k, (a, b) in enumerate(
                zip(hbm, (off_ref, type_ref, list_ref, chi_ref, eta_ref, gamma_ref))
            )
        ]
        me = {a: lax.axis_index(a) for a in AXES}
        side = 2 * (1 - lax.rem(me["gx"], 2)) if paired else 0

        def real(place):
            if paired and inside(place, (1, 2)) and place[0] != 1:
                return (side if place[0] == 0 else 2 - side,) + place[1:]
            return place

        def arrival(step):
            if step[2] > 0:
                return jnp.where(me["gz"] == sizes["gz"] - 1, 5, 2)
            if step[2] < 0:
                return jnp.where(me["gz"] == 1, 2, 5)
            if step[1]:
                return 1 if step[0] else 0
            if not paired:
                return 3 if step[0] > 0 else 4
            return jnp.where(side - 1 == step[0], 3, 4)

        def departure(step):
            if step[2]:
                return 2 if step[2] > 0 else 5
            if step[1]:
                return 1 if step[0] else 0
            return 3 if step[0] > 0 else 4

        pairs = [[] for _ in range(5)]
        for t, home in enumerate(local):
            split = [[], [], []]
            for step in STEPS:
                marked = tuple(h + 1 + d for h, d in zip(home, step))
                if reach(marked) == 3:
                    continue
                place = real(marked)
                n = ((place[0] - home[0]) * 3 + step[1] + 1) * 3 + step[2] + 1
                split[reach(marked)].append((n, place, step == (0, 0, 0)))
            for kept, part in zip(pairs, split):
                kept.append((t, part))
        edge = me["gz"] == 0
        far = (jnp.where(edge, cells[2] + 1, 0), jnp.where(edge, 0, cells[2] + 1))
        for which, pz in zip((3, 4), far):
            tz = jnp.where(pz == 0, 0, cells[2] - 1)
            for x, y in itertools.product(range(cells[0]), range(cells[1])):
                part = [
                    ((a * 3 + b) * 3 + pz - tz, (x + a, y + b, pz), False)
                    for a, b in itertools.product(range(3), repeat=2)
                ]
                pairs[which].append(((x * cells[1] + y) * cells[2] + tz, part))

        def places_of(which):
            if which < 3:
                return [real(p) for p in padded if reach(p) == which]
            return [p + (far[which - 3],) for p in itertools.product(*map(range, width[:2]))]

        def neighbour(step):
            return tuple(
                lax.rem(me[a] + (d + sizes[a]), sizes[a]) for a, d in zip(AXES, step)
            )

        def member(axes, hop):
            rank = 0
            count = 1
            for a in axes:
                rank = rank * sizes[a] + me[a]
                count = count * sizes[a]
            rank = lax.rem(rank + hop, count)
            place = dict(me)
            for a in reversed(axes):
                place[a] = lax.rem(rank, sizes[a])
                rank = rank // sizes[a]
            return tuple(place[a] for a in AXES)

        def lookup(kinds, table):
            result = jnp.zeros(kinds.shape, jnp.float32)
            for k in range(types):
                result = jnp.where(kinds == float(k), table[k], result)
            return result

        for load in loads[:2]:
            load.start()
        barrier = pltpu.get_barrier_semaphore()

        def greet(place):
            pl.semaphore_signal(barrier, inc=1, device_id=place, device_id_type=MESH)

        odd = lax.rem(me["gx"], 2)
        greeted = 0
        if planes:
            for dz in range(sizes["gz"]):
                for k, dy in itertools.product(range(sizes["gx"] // 2), range(sizes["gy"])):
                    x = me["gx"] - odd + 2 * k + (1 if dz else 0)
                    place = (
                        lax.rem(x, sizes["gx"]),
                        lax.rem(me["gy"] + dy, sizes["gy"]),
                        lax.rem(me["gz"] + dz, sizes["gz"]),
                    )
                    if (dz, k, dy) == (0, 0, 0):
                        pl.when(odd == 1)(lambda place=place: greet(place))
                    else:
                        greet(place)
        else:
            for axes, count in zip(groups, group_sizes):
                for hop in range(1, count):
                    greet(member(axes, hop))
                    greeted += 1
            if len(groups) > 1:
                for step in REMOTE:
                    greet(neighbour(step))
                    greeted += 1

        def tell(which):
            partner = (me["gx"] + 1 - 2 * odd, me["gy"], me["gz"])
            pl.semaphore_signal(met.at[which], inc=1, device_id=partner, device_id_type=MESH)

        def plane_is_in():
            @pl.when(odd == 0)
            def _():
                pl.semaphore_wait(barrier, sizes["gx"] * sizes["gy"] - 1)
                tell(0)

            @pl.when(odd == 1)
            def _():
                pl.semaphore_wait(met.at[0], 1)

        def others_are_in():
            @pl.when(odd == 1)
            def _():
                pl.semaphore_wait(barrier, sizes["gx"] * sizes["gy"] * (sizes["gz"] - 1))
                tell(1)

            @pl.when(odd == 0)
            def _():
                pl.semaphore_wait(met.at[1], 1)

        for load in loads[2:]:
            load.start()
        for load in loads[:2]:
            load.wait()

        row4 = lax.broadcasted_iota(jnp.int32, (4, atoms), 0)

        def shifted(place):
            ends = [
                CELL_EDGE * (jnp.asarray(p, jnp.int32).astype(jnp.float32) - (1.0 + 0.5 * c))
                for p, c in zip(place, cells)
            ]
            return jnp.where(row4 == 0, ends[0], jnp.where(row4 == 1, ends[1], ends[2]))

        def stacked(raw, place):
            p = jnp.where(row4 < 3, (raw + shifted(place)) * (1.0 / CUTOFF), 0.0)
            return jnp.where(row4 < 3, p, jnp.sum(p * p, axis=0, keepdims=True))

        def thirds(values):
            pieces = []
            for k in range(3):
                piece = values.astype(jnp.bfloat16).astype(jnp.float32)
                pieces.append(piece)
                if k < 2:
                    values = values - piece
            return pieces

        def sigma(kinds):
            root = lax.rsqrt(lookup(kinds, gamma_ref))
            return root * root * root * (CUTOFF**-1.5)

        for x, y, z in local:
            for f in range(3):
                fields[x + 1, y + 1, z + 1, f : f + 1, :] = off_ref[f, x, y, z : z + 1, :]
            fields[x + 1, y + 1, z + 1, 3:4, :] = type_ref[x, y, z : z + 1, :].astype(jnp.float32)

        def locate(places):
            for place in places:
                x, y, z = place
                kinds = fields[x, y, z, 3:4, :]
                v1, v2, v3 = thirds(stacked(fields[x, y, z], place))
                unit = jnp.where(row4 < 3, 1.0, 0.0)
                geometry[x, y, z] = jnp.concatenate(
                    [v1, v2, v3, v1, v2, v1, unit, jnp.zeros_like(unit)], axis=0
                )
                shields[x, y, z, 0:1, :] = sigma(kinds)
                source[x, y, z, 0:1, :] = -lookup(kinds, chi_ref)
                source[x, y, z, 1:2, :] = jnp.full((1, atoms), -1.0, jnp.float32)

        with jax.named_scope("barrier"):
            if planes:
                plane_is_in()
            else:
                pl.semaphore_wait(barrier, greeted)

        def halo(buffer, stage, steps=REMOTE):
            for step in steps:
                here, there = rounded_sides(step, cells)
                pltpu.make_async_remote_copy(
                    src_ref=buffer.at[here],
                    dst_ref=buffer.at[there],
                    send_sem=halo_send.at[stage, departure(step)],
                    recv_sem=halo_recv.at[stage, arrival(step)],
                    device_id=neighbour(step),
                    device_id_type=MESH,
                ).start()

        def whole_kind(buffer, stage, kind):
            return pltpu.make_async_remote_copy(
                src_ref=buffer.at[boxes[kind]],
                dst_ref=buffer.at[boxes[kind]],
                send_sem=halo_send.at[stage, kind],
                recv_sem=halo_recv.at[stage, kind],
                device_id=neighbour(REMOTE[0]),
                device_id_type=MESH,
            )

        def arrived(buffer, stage, which):
            for kind in ((), (3,), (0, 1, 4) if paired else (0, 1, 3, 4), (2,), (5,))[which]:
                whole_kind(buffer, stage, kind).wait_recv()

        def coupling(t, n, place, at, own_part, itself):
            square = lax.dot_general(
                own_part[0][:, :32],
                geometry[place],
                (((1,), (0,)), ((), ())),
                preferred_element_type=jnp.float32,
            )
            if itself:
                i = lax.broadcasted_iota(jnp.int32, (rows, atoms), 0) + at
                j = lax.broadcasted_iota(jnp.int32, (rows, atoms), 1)
                square = jnp.where(i == j, 4.0, square)
            u = square * lax.rsqrt(square)
            w = jnp.maximum(listed[n, pl.ds(t, 1), :] - u, 0.0)
            w = w * w
            w = w * w
            shape = (u + 0.5) * (square + 0.2) - 0.05
            cube = square * u + own_part[1] * shields[place[0], place[1], place[2], 0:1, :]
            return w * shape * jnp.exp2(jnp.log2(cube) * (-1.0 / 3.0))

        lanes = lax.broadcasted_iota(jnp.int32, (rows, atoms), 1)

        def fold(first_half, second_half, shift):
            clear = (lanes & shift) == 0
            kept = jnp.where(clear, first_half, second_half)
            return kept + pltpu.roll(jnp.where(clear, second_half, first_half), shift, 1)

        def tile_pass(vector, groups_now, building):
            merged = [(t, list(part)) for t, part in pairs[groups_now[0]]]
            for which in groups_now[1:]:
                for (_, kept), (_, part) in zip(merged, pairs[which]):
                    kept.extend(part)

            def slab(index, carry):
                at = pl.multiple_of(index * rows, rows)
                for t, part in merged:
                    if 0 in groups_now:
                        total_s = jnp.zeros((rows, atoms), jnp.float32)
                        total_t = jnp.zeros((rows, atoms), jnp.float32)
                    else:
                        total_s = sums[t, 0, pl.ds(at, rows), :]
                        total_t = sums[t, 1, pl.ds(at, rows), :]
                    if building:
                        own_part = [columns[t, f, pl.ds(at, rows), :] for f in range(2)]
                    for n, (x, y, z), itself in part:
                        if building:
                            block = coupling(t, n, (x, y, z), at, own_part, itself)
                            blocks[t, n, pl.ds(at, rows), :] = block
                            total_t = total_t - block
                        else:
                            block = blocks[t, n, pl.ds(at, rows), :]
                            total_t = total_t + block * vector[x, y, z, 1:2, :]
                        total_s = total_s + block * vector[x, y, z, 0:1, :]
                    sums[t, 0, pl.ds(at, rows), :] = total_s
                    sums[t, 1, pl.ds(at, rows), :] = total_t
                return carry

            lax.fori_loop(0, atoms // rows, slab, 0)

        scale = 20.0 * COULOMB / CUTOFF
        high = max(16, 2 * tiles)
        sheaf = lax.broadcasted_iota(jnp.int32, (high, 3 * atoms), 1) % atoms // base
        gather = jnp.where(
            sheaf == lax.broadcasted_iota(jnp.int32, (high, 3 * atoms), 0), 1.0, 0.0
        ).astype(jnp.bfloat16)

        def collect(vector, image):
            folded = []
            for at in range(0, atoms, rows):
                left = [sums[t, k, at : at + rows, :] for t in range(tiles) for k in range(2)]
                shift = base
                while len(left) > 1:
                    left = [fold(a, b, shift) for a, b in zip(left[::2], left[1::2])]
                    shift = 2 * shift
                folded.append(left[0])
            left = jnp.concatenate(folded, axis=0)
            pieces = []
            for k in range(3):
                piece = left.astype(jnp.bfloat16)
                pieces.append(piece)
                if k < 2:
                    left = left - piece.astype(jnp.float32)
            result = lax.dot_general(
                gather,
                jnp.concatenate(pieces, axis=1),
                (((1,), (1,)), ((), ())),
                preferred_element_type=jnp.float32,
            )
            for t, (x, y, z) in enumerate(local):
                here = vector[x + 1, y + 1, z + 1]
                image(x, y, z, eta[t] * here + scale * result[2 * t : 2 * t + 2])

        def to_padded(buffer):
            def store(x, y, z, pair):
                buffer[x + 1, y + 1, z + 1] = pair

            return store

        def to_own(x, y, z, pair):
            own_image[x, y, z] = pair

        lane = lax.broadcasted_iota(jnp.int32, (2, atoms), 1)

        def over_own(values):
            return jnp.sum(jnp.sum(values, axis=(0, 1, 2)), axis=1, keepdims=True)

        def sum_copies(g, stage):
            axes, count = groups[g], group_sizes[g]
            return [
                pltpu.make_async_remote_copy(
                    src_ref=parts[g].at[stage, 0],
                    dst_ref=parts[g].at[stage, hop],
                    send_sem=sum_send.at[stage, g],
                    recv_sem=sum_recv.at[stage, g],
                    device_id=member(axes, hop),
                    device_id_type=MESH,
                )
                for hop in range(1, count)
            ]

        def whole_sum(g, stage):
            count = group_sizes[g]
            return pltpu.make_async_remote_copy(
                src_ref=parts[g].at[stage, pl.ds(1, count - 1)],
                dst_ref=parts[g].at[stage, pl.ds(1, count - 1)],
                send_sem=sum_send.at[stage, g],
                recv_sem=sum_recv.at[stage, g],
                device_id=member(groups[g], 1),
                device_id_type=MESH,
            )

        def start_sums(values, stage):
            message = jnp.zeros((2, atoms), jnp.float32)
            for k, value in enumerate(values):
                message = jnp.where(lane == k, value, message)
            parts[0][stage, 0] = message
            for copy in sum_copies(0, stage):
                copy.start()

        def finish_sums(number, stage):
            for g in range(len(groups)):
                whole_sum(g, stage).wait_recv()
                total = jnp.sum(parts[g][stage], axis=0)
                if g + 1 < len(groups):
                    parts[g + 1][stage, 0] = total
                    for copy in sum_copies(g + 1, stage):
                        copy.start()
            return [
                jnp.sum(jnp.where(lane == k, total, 0.0), axis=1, keepdims=True)
                for k in range(number)
            ]

        def distant_positions():
            others_are_in()
            halo(fields, 0, DISTANT)

        last = me["gz"] == sizes["gz"] - 1
        if planes:
            halo(fields, 0, CLOSE)
            pl.when(last)(distant_positions)
        else:
            halo(fields, 0)
        for load in loads[2:]:
            load.wait()
        locate(places_of(0))
        for t, (x, y, z) in enumerate(local):
            place = (x + 1, y + 1, z + 1)
            v1, v2, v3 = thirds(stacked(fields[place], place))
            c1 = jnp.where(row4 < 3, -2.0 * v1, 1.0)
            c2 = jnp.where(row4 < 3, -2.0 * v2, 0.0)
            c3 = jnp.where(row4 < 3, -2.0 * v3, 0.0)
            norms = jnp.where(
                row4 == 0, v1[3:4], jnp.where(row4 == 1, v2[3:4], jnp.where(row4 == 2, v3[3:4], 0.0))
            )
            none = jnp.zeros((atoms - 28, atoms), jnp.float32)
            columns[t, 0] = jnp.transpose(
                jnp.concatenate([c1, c1, c1, c2, c2, c3, norms, none], axis=0)
            )
            row = shields[x + 1, y + 1, z + 1, 0:1, :]
            columns[t, 1] = jnp.transpose(jnp.broadcast_to(row, (atoms, atoms)))
        entries = jnp.concatenate(
            [list_ref[x, y, z : z + 1, :] - linear((x + 1, y + 1, z + 1)) for x, y, z in local], 0
        )
        for n, step in enumerate(STEPS):
            found = jnp.max(
                jnp.where(entries == linear(step), 1.0, 0.0), axis=1, keepdims=True
            )
            listed[n] = jnp.broadcast_to(1.0 - (1.0 - found) * FAR, (tiles, atoms))
        eta = [lookup(fields[x + 1, y + 1, z + 1, 3:4, :], eta_ref) for x, y, z in local]

        with jax.named_scope("build0"):
            tile_pass(source, (0,), True)
        for which in (1, 2, 3, 4) if paired else (2, 3, 4):
            if which == 2 and planes:
                with jax.named_scope("others"):
                    pl.when(jnp.logical_not(last))(distant_positions)
            with jax.named_scope(f"wait_pos{which}"):
                arrived(fields, 0, which)
            locate(places_of(which))
            with jax.named_scope(f"build{which}"):
                tile_pass(source, (which,), True)
        with jax.named_scope("collect0"):
            collect(source, to_padded(first))

        def apply(vector, stage, number):
            with jax.named_scope(f"pass{stage}_0"):
                tile_pass(vector, (0,), False)
            with jax.named_scope(f"wait{stage}_1"):
                if paired:
                    arrived(vector, stage, 1)
                arrived(vector, stage, 2)
            with jax.named_scope(f"pass{stage}_1"):
                tile_pass(vector, (1, 2) if paired else (2,), False)
            for which in (3, 4):
                with jax.named_scope(f"wait{stage}_{which}"):
                    arrived(vector, stage, which)
                with jax.named_scope(f"pass{stage}_{which}"):
                    tile_pass(vector, (which,), False)
            with jax.named_scope(f"sums{stage}"):
                totals = finish_sums(number, stage - 1)
            collect(vector, to_own)
            return totals

        residual = source[own]
        image = first[own]
        values = [over_own(residual * residual), over_own(residual * image)]
        halo(first, 1, DISTANT)
        start_sums(values, 0)
        halo(first, 1, CLOSE)
        norm_now, curvature = apply(first, 1, 2)
        step_size = norm_now / curvature
        direction, along = residual, image
        further = own_image[...]
        answer = step_size * direction
        residual = residual - step_size * along
        image = image - step_size * further
        second[own] = image
        values = [over_own(residual * residual), over_own(residual * image)]
        halo(second, 2, DISTANT)
        start_sums(values, 1)
        halo(second, 2, CLOSE)
        norm_next, curvature = apply(second, 2, 2)
        growth = norm_next / norm_now
        step_size = norm_next / (curvature - growth * norm_next / step_size)
        norm_now = norm_next
        further = own_image[...] + growth * further
        direction = residual + growth * direction
        along = image + growth * along
        answer = answer + step_size * direction
        residual = residual - step_size * along
        image = image - step_size * further
        values = [residual * residual, residual * image, answer, residual, direction]
        start_sums([over_own(v) for v in values], 2)
        with jax.named_scope("sums2"):
            norm_next, curvature, *others = finish_sums(5, 2)
        growth = norm_next / norm_now
        step_size = norm_next / (curvature - growth * norm_next / step_size)
        answer = answer + step_size * (residual + growth * direction)
        residual = residual - step_size * (image + growth * along)
        totals = others[0] + step_size * (others[1] + growth * others[2])
        level = totals[0:1] / totals[1:2]
        for x, y, z in local:
            charge_ref[x, y, z : z + 1, :] = 1000.0 * (
                answer[x, y, z, 0:1] - level * answer[x, y, z, 1:2]
            )
            for s in range(2):
                resid_ref[s, x, y, z : z + 1, :] = residual[x, y, z, s : s + 1]
        with jax.named_scope("drain"):
            for stage, buffer in enumerate((fields, first, second)):
                for kind in range(KINDS):
                    whole_kind(buffer, stage, kind).wait_send()
            for stage in range(ITERS):
                for g in range(len(groups)):
                    whole_sum(g, stage).wait_send()

    scratch = [
        pltpu.VMEM((3,) + cells + (atoms,), jnp.float32),
        pltpu.VMEM(cells + (atoms,), jnp.int32),
        None,
        pltpu.SMEM((types,), jnp.float32),
        pltpu.SMEM((types,), jnp.float32),
        pltpu.SMEM((types,), jnp.float32),
        pltpu.VMEM(width + (4, atoms), jnp.float32),
        pltpu.VMEM(width + (32, atoms), jnp.float32),
        pltpu.VMEM(width + (1, atoms), jnp.float32),
        pltpu.VMEM((tiles, 2, atoms, atoms), jnp.float32),
        pltpu.VMEM((len(STEPS), tiles, atoms), jnp.float32),
        pltpu.VMEM((tiles, len(STEPS), atoms, atoms), jnp.float32),
        pltpu.VMEM((tiles, 2, atoms, atoms), jnp.float32),
        pltpu.VMEM(width + (2, atoms), jnp.float32),
        pltpu.VMEM(width + (2, atoms), jnp.float32),
        pltpu.VMEM(width + (2, atoms), jnp.float32),
        pltpu.VMEM(cells + (2, atoms), jnp.float32),
    ]
    scratch += [pltpu.VMEM((ITERS, count, 2, atoms), jnp.float32) for count in group_sizes]
    scratch += [
        pltpu.SemaphoreType.DMA((6,)),
        pltpu.SemaphoreType.DMA((ITERS, KINDS)),
        pltpu.SemaphoreType.DMA((ITERS, KINDS)),
        pltpu.SemaphoreType.DMA((ITERS, len(groups))),
        pltpu.SemaphoreType.DMA((ITERS, len(groups))),
        pltpu.SemaphoreType.REGULAR((2,)),
    ]
    return kernel, scratch


def put_out(charge_in, resid_in, charge_ref, resid_ref, sems):
    copies = [
        pltpu.make_async_copy(charge_in, charge_ref, sems.at[0]),
        pltpu.make_async_copy(resid_in, resid_ref, sems.at[1]),
    ]
    for copy in copies:
        copy.start()
    for copy in copies:
        copy.wait()


def solution(mesh):
    sizes = {a: mesh.shape[a] for a in AXES}
    devices = sizes["gx"] * sizes["gy"] * sizes["gz"]
    groups = (AXES,) if devices <= 64 else tuple((a,) for a in AXES)

    def per_device(offsets, type_ids, neighbours, type_chi, type_eta, type_gamma):
        cells = offsets.shape[1:4]
        atoms = offsets.shape[4]
        types = type_chi.shape[0]
        kernel, scratch = make_kernel(sizes, groups, cells, atoms, types, 128)
        scratch[2] = pltpu.VMEM(neighbours.shape, jnp.int32)
        vmem = pl.BlockSpec(memory_space=pltpu.VMEM)
        hbm = pl.BlockSpec(memory_space=pltpu.HBM)
        pair = pl.pallas_call(
            kernel,
            out_shape=(
                jax.ShapeDtypeStruct(cells + (atoms,), jnp.float32),
                jax.ShapeDtypeStruct((2,) + cells + (atoms,), jnp.float32),
            ),
            in_specs=[hbm] * 6,
            out_specs=(vmem, vmem),
            scratch_shapes=scratch,
            compiler_params=pltpu.CompilerParams(
                collective_id=0, has_side_effects=True, vmem_limit_bytes=48 * 1024 * 1024
            ),
        )(*[pltpu.with_memory_space_constraint(v, pltpu.HBM) for v in (offsets, type_ids, neighbours, type_chi, type_eta, type_gamma)])
        return pl.pallas_call(
            put_out,
            out_shape=tuple(jax.ShapeDtypeStruct(v.shape, v.dtype) for v in pair),
            in_specs=[vmem] * 2,
            out_specs=(hbm, hbm),
            scratch_shapes=[pltpu.SemaphoreType.DMA((2,))],
        )(*[pltpu.with_memory_space_constraint(v, pltpu.VMEM) for v in pair])

    placed = (
        P(None, "gx", "gy", "gz", None),
        P("gx", "gy", "gz", None),
        P("gx", "gy", "gz", None),
        P(),
        P(),
        P(),
    )
    return jax.shard_map(
        per_device,
        mesh=mesh,
        in_specs=placed,
        out_specs=(P("gx", "gy", "gz", None), P(None, "gx", "gy", "gz", None)),
        check_vma=False,
    )
```

```python
import itertools

import jax
import jax.numpy as jnp
from jax import lax
from jax.experimental import pallas as pl
from jax.experimental.pallas import tpu as pltpu
from jax.sharding import PartitionSpec as P

ITERS = 3
CELL_EDGE = 11.0
CUTOFF = 10.0
COULOMB = 14.4
AXES = ("gx", "gy", "gz")
FAR = 1000.0
MESH = pl.DeviceIdType.MESH
STEPS = [d for d in itertools.product((-1, 0, 1), repeat=3)]
REMOTE = sorted((d for d in STEPS if d != (0, 0, 0)), key=lambda d: (-abs(d[2]), -abs(d[0])))
KINDS = 6


def make_kernel(sizes, groups, cells, atoms, types, rows):
    width = tuple(c + 2 for c in cells)
    tiles = cells[0] * cells[1] * cells[2]
    local = list(itertools.product(*[range(c) for c in cells]))
    padded = list(itertools.product(*[range(w) for w in width]))
    own = (slice(1, 1 + cells[0]), slice(0, cells[1]), slice(1, 1 + cells[2]))
    joined = sizes["gy"] == 2 and cells[1] == 2
    steps = [d for d in REMOTE if not (joined and d[1] < 0)]
    distant = [d for d in steps if d[2]]
    close = [d for d in steps if not d[2]]

    def slot(place):
        return (place[0], (place[1] - 1) % width[1], place[2])

    def rounded_sides(step):
        source, target = [], []
        for axis, (d, c) in enumerate(zip(step, cells)):
            first, low, high = (0, c + 1, c) if axis == 1 else (1, 0, c + 1)
            if d == 0:
                source.append(pl.ds(first, c))
                target.append(pl.ds(first, c))
            elif axis == 1 and joined:
                source.append(pl.ds(0, 2))
                target.append(pl.ds(2, 2))
            elif d > 0:
                source.append(pl.ds(first + c - 1, 1))
                target.append(pl.ds(low, 1))
            else:
                source.append(pl.ds(first, 1))
                target.append(pl.ds(high, 1))
        return tuple(source), tuple(target)

    group_sizes = []
    for axes in groups:
        count = 1
        for a in axes:
            count = count * sizes[a]
        group_sizes.append(count)
    boxes = (
        (pl.ds(0, cells[0]), pl.ds(0, 2), pl.ds(0, cells[2])),
        (pl.ds(0, 2), pl.ds(0, 2), pl.ds(0, cells[2])),
        (pl.ds(0, width[0]), pl.ds(0, width[1]), pl.ds(0, 1)),
        (pl.ds(0, 1), pl.ds(0, cells[1]), pl.ds(0, cells[2])),
        (pl.ds(0, 1), pl.ds(0, cells[1]), pl.ds(0, cells[2])),
        (pl.ds(0, width[0]), pl.ds(0, width[1]), pl.ds(0, 1)),
    )
    paired = cells[0] == 1 and sizes["gx"] % 2 == 0
    planes = paired and len(groups) == 1
    base = atoms // (2 * tiles)

    def linear(place):
        return (place[0] * width[1] + place[1]) * width[2] + place[2]

    def inside(place, axes):
        return all(1 <= place[a] <= cells[a] for a in axes)

    def reach(place):
        if inside(place, (0, 1, 2)):
            return 0
        if not inside(place, (2,)):
            return 3
        return 1 if paired and inside(place, (1,)) and place[0] == 0 else 2

    def kernel(*refs):
        hbm, (charge_ref, resid_ref) = refs[:6], refs[6:8]
        (off_ref, type_ref, list_ref, chi_ref, eta_ref, gamma_ref) = refs[8:14]
        (fields, geometry, shields, columns, listed, blocks, sums, source) = refs[14:22]
        (first, second, own_image) = refs[22:25]
        parts = refs[25 : 25 + len(groups)]
        load_sem, halo_send, halo_recv, sum_send, sum_recv, met = refs[25 + len(groups) :]

        loads = [
            pltpu.make_async_copy(a, b, load_sem.at[k])
            for k, (a, b) in enumerate(
                zip(hbm, (off_ref, type_ref, list_ref, chi_ref, eta_ref, gamma_ref))
            )
        ]
        me = {a: lax.axis_index(a) for a in AXES}
        side = 2 * (1 - lax.rem(me["gx"], 2)) if paired else 0

        def real(place):
            if paired and inside(place, (1, 2)) and place[0] != 1:
                return (side if place[0] == 0 else 2 - side,) + place[1:]
            return place

        upward = jnp.where(me["gz"] == sizes["gz"] - 1, 5, 2)
        downward = jnp.where(me["gz"] == 1, 2, 5)
        eastward = jnp.where(side == 2, 3, 4)
        westward = jnp.where(side == 2, 4, 3)

        def arrival(step):
            if step[2]:
                return upward if step[2] > 0 else downward
            if step[1]:
                return 1 if step[0] else 0
            if not paired:
                return 3 if step[0] > 0 else 4
            return eastward if step[0] > 0 else westward

        def departure(step):
            if step[2]:
                return 2 if step[2] > 0 else 5
            if step[1]:
                return 1 if step[0] else 0
            return 3 if step[0] > 0 else 4

        pairs = [[] for _ in range(5)]
        for t, home in enumerate(local):
            split = [[], [], []]
            for step in STEPS:
                marked = tuple(h + 1 + d for h, d in zip(home, step))
                if reach(marked) == 3:
                    continue
                place = real(marked)
                n = ((place[0] - home[0]) * 3 + step[1] + 1) * 3 + step[2] + 1
                split[reach(marked)].append((n, place, step == (0, 0, 0)))
            for kept, part in zip(pairs, split):
                kept.append((t, part))
        edge = me["gz"] == 0
        far = (jnp.where(edge, cells[2] + 1, 0), jnp.where(edge, 0, cells[2] + 1))
        for which, pz in zip((3, 4), far):
            tz = jnp.where(pz == 0, 0, cells[2] - 1)
            for x, y in itertools.product(range(cells[0]), range(cells[1])):
                part = [
                    ((a * 3 + b) * 3 + pz - tz, (x + a, y + b, pz), False)
                    for a, b in itertools.product(range(3), repeat=2)
                ]
                pairs[which].append(((x * cells[1] + y) * cells[2] + tz, part))

        def places_of(which):
            if which < 3:
                return [real(p) for p in padded if reach(p) == which]
            return [p + (far[which - 3],) for p in itertools.product(*map(range, width[:2]))]

        turned = {
            a: [lax.rem(me[a] + d, sizes[a]) if d else me[a] for d in range(sizes[a])] for a in AXES
        }

        def neighbour(step):
            return tuple(turned[a][d % sizes[a]] for a, d in zip(AXES, step))

        def member(axes, hop):
            place = dict(me)
            for a in reversed(axes):
                place[a] = turned[a][hop % sizes[a]]
                hop = hop // sizes[a]
            return tuple(place[a] for a in AXES)

        def lookup(kinds, table):
            result = jnp.zeros(kinds.shape, jnp.float32)
            for k in range(types):
                result = jnp.where(kinds == float(k), table[k], result)
            return result

        for load in loads[:2]:
            load.start()
        barrier = pltpu.get_barrier_semaphore()

        def greet(place):
            pl.semaphore_signal(barrier, inc=1, device_id=place, device_id_type=MESH)

        odd = lax.rem(me["gx"], 2)
        greeted = 0
        if planes:
            for dz in range(sizes["gz"]):
                for k, dy in itertools.product(range(sizes["gx"] // 2), range(sizes["gy"])):
                    x = me["gx"] - odd + 2 * k + (1 if dz else 0)
                    place = (
                        lax.rem(x, sizes["gx"]),
                        lax.rem(me["gy"] + dy, sizes["gy"]),
                        lax.rem(me["gz"] + dz, sizes["gz"]),
                    )
                    if (dz, k, dy) == (0, 0, 0):
                        pl.when(odd == 1)(lambda place=place: greet(place))
                    else:
                        greet(place)
        else:
            for axes, count in zip(groups, group_sizes):
                for hop in range(1, count):
                    greet(member(axes, hop))
                    greeted += 1
            if len(groups) > 1:
                for step in REMOTE:
                    greet(neighbour(step))
                    greeted += 1

        def tell(which):
            partner = (me["gx"] + 1 - 2 * odd, me["gy"], me["gz"])
            pl.semaphore_signal(met.at[which], inc=1, device_id=partner, device_id_type=MESH)

        def plane_is_in():
            @pl.when(odd == 0)
            def _():
                pl.semaphore_wait(barrier, sizes["gx"] * sizes["gy"] - 1)
                tell(0)

            @pl.when(odd == 1)
            def _():
                pl.semaphore_wait(met.at[0], 1)

        def others_are_in():
            @pl.when(odd == 1)
            def _():
                pl.semaphore_wait(barrier, sizes["gx"] * sizes["gy"] * (sizes["gz"] - 1))
                tell(1)

            @pl.when(odd == 0)
            def _():
                pl.semaphore_wait(met.at[1], 1)

        for load in loads[2:]:
            load.start()
        for load in loads[:2]:
            load.wait()

        row4 = lax.broadcasted_iota(jnp.int32, (4, atoms), 0)

        def shifted(place):
            ends = [
                CELL_EDGE * (jnp.asarray(p, jnp.int32).astype(jnp.float32) - (1.0 + 0.5 * c))
                for p, c in zip(place, cells)
            ]
            return jnp.where(row4 == 0, ends[0], jnp.where(row4 == 1, ends[1], ends[2]))

        def stacked(raw, place):
            p = jnp.where(row4 < 3, (raw + shifted(place)) * (1.0 / CUTOFF), 0.0)
            return jnp.where(row4 < 3, p, jnp.sum(p * p, axis=0, keepdims=True))

        def thirds(values):
            pieces = []
            for k in range(3):
                piece = values.astype(jnp.bfloat16).astype(jnp.float32)
                pieces.append(piece)
                if k < 2:
                    values = values - piece
            return pieces

        def sigma(kinds):
            root = lax.rsqrt(lookup(kinds, gamma_ref))
            return root * root * root * (CUTOFF**-1.5)

        for x, y, z in local:
            for f in range(3):
                fields[x + 1, y, z + 1, f : f + 1, :] = off_ref[f, x, y, z : z + 1, :]
            fields[x + 1, y, z + 1, 3:4, :] = type_ref[x, y, z : z + 1, :].astype(jnp.float32)

        def locate(places):
            for place in places:
                x, y, z = slot(place)
                kinds = fields[x, y, z, 3:4, :]
                v1, v2, v3 = thirds(stacked(fields[x, y, z], place))
                unit = jnp.where(row4 < 3, 1.0, 0.0)
                geometry[x, y, z] = jnp.concatenate(
                    [v1, v2, v3, v1, v2, v1, unit, jnp.zeros_like(unit)], axis=0
                )
                shields[x, y, z, 0:1, :] = sigma(kinds)
                source[x, y, z, 0:1, :] = -lookup(kinds, chi_ref)
                source[x, y, z, 1:2, :] = jnp.full((1, atoms), -1.0, jnp.float32)

        with jax.named_scope("barrier"):
            if planes:
                plane_is_in()
            else:
                pl.semaphore_wait(barrier, greeted)

        def halo(buffer, stage, chosen):
            for step in chosen:
                here, there = rounded_sides(step)
                pltpu.make_async_remote_copy(
                    src_ref=buffer.at[here],
                    dst_ref=buffer.at[there],
                    send_sem=halo_send.at[stage, departure(step)],
                    recv_sem=halo_recv.at[stage, arrival(step)],
                    device_id=neighbour(step),
                    device_id_type=MESH,
                ).start()

        def whole_kind(buffer, stage, kind):
            return pltpu.make_async_remote_copy(
                src_ref=buffer.at[boxes[kind]],
                dst_ref=buffer.at[boxes[kind]],
                send_sem=halo_send.at[stage, kind],
                recv_sem=halo_recv.at[stage, kind],
                device_id=neighbour(REMOTE[0]),
                device_id_type=MESH,
            )

        def arrived(buffer, stage, which):
            for kind in ((), (3,), (0, 1, 4) if paired else (0, 1, 3, 4), (2,), (5,))[which]:
                whole_kind(buffer, stage, kind).wait_recv()

        def coupling(t, n, place, at, own_part, itself):
            x, y, z = place
            square = lax.dot_general(
                own_part[0][:, :32],
                geometry[x, y, z],
                (((1,), (0,)), ((), ())),
                preferred_element_type=jnp.float32,
            )
            if itself:
                i = lax.broadcasted_iota(jnp.int32, (rows, atoms), 0) + at
                j = lax.broadcasted_iota(jnp.int32, (rows, atoms), 1)
                square = jnp.where(i == j, 4.0, square)
            u = square * lax.rsqrt(square)
            w = jnp.maximum(listed[n, pl.ds(t, 1), :] - u, 0.0)
            w = w * w
            w = w * w
            shape = (u + 0.5) * (square + 0.2) - 0.05
            cube = square * u + own_part[1] * shields[x, y, z, 0:1, :]
            return w * shape * jnp.exp2(jnp.log2(cube) * (-1.0 / 3.0))

        lanes = lax.broadcasted_iota(jnp.int32, (rows, atoms), 1)

        def fold(first_half, second_half, shift):
            clear = (lanes & shift) == 0
            kept = jnp.where(clear, first_half, second_half)
            return kept + pltpu.roll(jnp.where(clear, second_half, first_half), shift, 1)

        def tile_pass(vector, groups_now, building):
            merged = [(t, list(part)) for t, part in pairs[groups_now[0]]]
            for which in groups_now[1:]:
                for (_, kept), (_, part) in zip(merged, pairs[which]):
                    kept.extend(part)

            def slab(index, carry):
                at = pl.multiple_of(index * rows, rows)
                for t, part in merged:
                    if 0 in groups_now:
                        total_s = jnp.zeros((rows, atoms), jnp.float32)
                        total_t = jnp.zeros((rows, atoms), jnp.float32)
                    else:
                        total_s = sums[t, 0, pl.ds(at, rows), :]
                        total_t = sums[t, 1, pl.ds(at, rows), :]
                    if building:
                        own_part = [columns[t, f, pl.ds(at, rows), :] for f in range(2)]
                    for n, place, itself in part:
                        x, y, z = slot(place)
                        if building:
                            block = coupling(t, n, (x, y, z), at, own_part, itself)
                            blocks[t, n, pl.ds(at, rows), :] = block
                            total_t = total_t - block
                        else:
                            block = blocks[t, n, pl.ds(at, rows), :]
                            total_t = total_t + block * vector[x, y, z, 1:2, :]
                        total_s = total_s + block * vector[x, y, z, 0:1, :]
                    sums[t, 0, pl.ds(at, rows), :] = total_s
                    sums[t, 1, pl.ds(at, rows), :] = total_t
                return carry

            lax.fori_loop(0, atoms // rows, slab, 0)

        scale = 20.0 * COULOMB / CUTOFF
        high = max(16, 2 * tiles)
        sheaf = lax.broadcasted_iota(jnp.int32, (high, 3 * atoms), 1) % atoms // base
        gather = jnp.where(
            sheaf == lax.broadcasted_iota(jnp.int32, (high, 3 * atoms), 0), 1.0, 0.0
        ).astype(jnp.bfloat16)

        def collect(vector, image):
            folded = []
            for at in range(0, atoms, rows):
                left = [sums[t, k, at : at + rows, :] for t in range(tiles) for k in range(2)]
                shift = base
                while len(left) > 1:
                    left = [fold(a, b, shift) for a, b in zip(left[::2], left[1::2])]
                    shift = 2 * shift
                folded.append(left[0])
            left = jnp.concatenate(folded, axis=0)
            pieces = []
            for k in range(3):
                piece = left.astype(jnp.bfloat16)
                pieces.append(piece)
                if k < 2:
                    left = left - piece.astype(jnp.float32)
            result = lax.dot_general(
                gather,
                jnp.concatenate(pieces, axis=1),
                (((1,), (1,)), ((), ())),
                preferred_element_type=jnp.float32,
            )
            for t, (x, y, z) in enumerate(local):
                here = vector[x + 1, y, z + 1]
                image(x, y, z, eta[t] * here + scale * result[2 * t : 2 * t + 2])

        def to_padded(buffer):
            def store(x, y, z, pair):
                buffer[x + 1, y, z + 1] = pair

            return store

        def to_own(x, y, z, pair):
            own_image[x, y, z] = pair

        lane = lax.broadcasted_iota(jnp.int32, (2, atoms), 1)

        def over_own(values):
            return jnp.sum(jnp.sum(values, axis=(0, 1, 2)), axis=1, keepdims=True)

        def sum_copies(g, stage):
            axes, count = groups[g], group_sizes[g]
            return [
                pltpu.make_async_remote_copy(
                    src_ref=parts[g].at[stage, 0],
                    dst_ref=parts[g].at[stage, hop],
                    send_sem=sum_send.at[stage, g],
                    recv_sem=sum_recv.at[stage, g],
                    device_id=member(axes, hop),
                    device_id_type=MESH,
                )
                for hop in range(1, count)
            ]

        def whole_sum(g, stage):
            count = group_sizes[g]
            return pltpu.make_async_remote_copy(
                src_ref=parts[g].at[stage, pl.ds(1, count - 1)],
                dst_ref=parts[g].at[stage, pl.ds(1, count - 1)],
                send_sem=sum_send.at[stage, g],
                recv_sem=sum_recv.at[stage, g],
                device_id=member(groups[g], 1),
                device_id_type=MESH,
            )

        def start_sums(values, stage):
            message = jnp.zeros((2, atoms), jnp.float32)
            for k, value in enumerate(values):
                message = jnp.where(lane == k, value, message)
            parts[0][stage, 0] = message
            for copy in sum_copies(0, stage):
                copy.start()

        def finish_sums(number, stage):
            for g in range(len(groups)):
                whole_sum(g, stage).wait_recv()
                total = jnp.sum(parts[g][stage], axis=0)
                if g + 1 < len(groups):
                    parts[g + 1][stage, 0] = total
                    for copy in sum_copies(g + 1, stage):
                        copy.start()
            return [
                jnp.sum(jnp.where(lane == k, total, 0.0), axis=1, keepdims=True)
                for k in range(number)
            ]

        def distant_positions():
            others_are_in()
            halo(fields, 0, distant)

        last = me["gz"] == sizes["gz"] - 1
        if planes:
            halo(fields, 0, close)
            pl.when(last)(distant_positions)
        else:
            halo(fields, 0, steps)
        for load in loads[2:]:
            load.wait()
        locate(places_of(0))
        for t, (x, y, z) in enumerate(local):
            place = (x + 1, y + 1, z + 1)
            v1, v2, v3 = thirds(stacked(fields[slot(place)], place))
            c1 = jnp.where(row4 < 3, -2.0 * v1, 1.0)
            c2 = jnp.where(row4 < 3, -2.0 * v2, 0.0)
            c3 = jnp.where(row4 < 3, -2.0 * v3, 0.0)
            norms = jnp.where(
                row4 == 0, v1[3:4], jnp.where(row4 == 1, v2[3:4], jnp.where(row4 == 2, v3[3:4], 0.0))
            )
            none = jnp.zeros((atoms - 28, atoms), jnp.float32)
            columns[t, 0] = jnp.transpose(
                jnp.concatenate([c1, c1, c1, c2, c2, c3, norms, none], axis=0)
            )
            row = shields[x + 1, y, z + 1, 0:1, :]
            columns[t, 1] = jnp.transpose(jnp.broadcast_to(row, (atoms, atoms)))
        entries = jnp.concatenate(
            [list_ref[x, y, z : z + 1, :] - linear((x + 1, y + 1, z + 1)) for x, y, z in local], 0
        )
        for n, step in enumerate(STEPS):
            found = jnp.max(
                jnp.where(entries == linear(step), 1.0, 0.0), axis=1, keepdims=True
            )
            listed[n] = jnp.broadcast_to(1.0 - (1.0 - found) * FAR, (tiles, atoms))
        eta = [lookup(fields[x + 1, y, z + 1, 3:4, :], eta_ref) for x, y, z in local]

        with jax.named_scope("build0"):
            tile_pass(source, (0,), True)
        for which in (1, 2, 3, 4) if paired else (2, 3, 4):
            if which == 2 and planes:
                with jax.named_scope("others"):
                    pl.when(jnp.logical_not(last))(distant_positions)
            with jax.named_scope(f"wait_pos{which}"):
                arrived(fields, 0, which)
            locate(places_of(which))
            with jax.named_scope(f"build{which}"):
                tile_pass(source, (which,), True)
        with jax.named_scope("collect0"):
            collect(source, to_padded(first))

        def apply(vector, stage, number):
            with jax.named_scope(f"pass{stage}_0"):
                tile_pass(vector, (0,), False)
            with jax.named_scope(f"wait{stage}_1"):
                if paired:
                    arrived(vector, stage, 1)
                arrived(vector, stage, 2)
            with jax.named_scope(f"pass{stage}_1"):
                tile_pass(vector, (1, 2) if paired else (2,), False)
            for which in (3, 4):
                with jax.named_scope(f"wait{stage}_{which}"):
                    arrived(vector, stage, which)
                with jax.named_scope(f"pass{stage}_{which}"):
                    tile_pass(vector, (which,), False)
            with jax.named_scope(f"collect{stage}"):
                collect(vector, to_own)
            with jax.named_scope(f"sums{stage}"):
                return finish_sums(number, stage - 1)

        residual = source[own]
        image = first[own]
        values = [over_own(residual * residual), over_own(residual * image)]
        halo(first, 1, distant)
        start_sums(values, 0)
        halo(first, 1, close)
        norm_now, curvature = apply(first, 1, 2)
        step_size = norm_now / curvature
        direction, along = residual, image
        further = own_image[...]
        answer = step_size * direction
        residual = residual - step_size * along
        image = image - step_size * further
        second[own] = image
        values = [over_own(residual * residual), over_own(residual * image)]
        halo(second, 2, distant)
        start_sums(values, 1)
        halo(second, 2, close)
        norm_next, curvature = apply(second, 2, 2)
        growth = norm_next / norm_now
        step_size = norm_next / (curvature - growth * norm_next / step_size)
        norm_now = norm_next
        further = own_image[...] + growth * further
        direction = residual + growth * direction
        along = image + growth * along
        answer = answer + step_size * direction
        residual = residual - step_size * along
        image = image - step_size * further
        values = [residual * residual, residual * image, answer, residual, direction]
        start_sums([over_own(v) for v in values], 2)
        with jax.named_scope("sums2"):
            norm_next, curvature, *others = finish_sums(5, 2)
        growth = norm_next / norm_now
        step_size = norm_next / (curvature - growth * norm_next / step_size)
        answer = answer + step_size * (residual + growth * direction)
        residual = residual - step_size * (image + growth * along)
        totals = others[0] + step_size * (others[1] + growth * others[2])
        level = totals[0:1] / totals[1:2]
        for x, y, z in local:
            charge_ref[x, y, z : z + 1, :] = 1000.0 * (
                answer[x, y, z, 0:1] - level * answer[x, y, z, 1:2]
            )
            for s in range(2):
                resid_ref[s, x, y, z : z + 1, :] = residual[x, y, z, s : s + 1]
        with jax.named_scope("drain"):
            for stage, buffer in enumerate((fields, first, second)):
                for kind in range(KINDS):
                    whole_kind(buffer, stage, kind).wait_send()
            for stage in range(ITERS):
                for g in range(len(groups)):
                    whole_sum(g, stage).wait_send()

    scratch = [
        pltpu.VMEM((3,) + cells + (atoms,), jnp.float32),
        pltpu.VMEM(cells + (atoms,), jnp.int32),
        None,
        pltpu.SMEM((types,), jnp.float32),
        pltpu.SMEM((types,), jnp.float32),
        pltpu.SMEM((types,), jnp.float32),
        pltpu.VMEM(width + (4, atoms), jnp.float32),
        pltpu.VMEM(width + (32, atoms), jnp.float32),
        pltpu.VMEM(width + (1, atoms), jnp.float32),
        pltpu.VMEM((tiles, 2, atoms, atoms), jnp.float32),
        pltpu.VMEM((len(STEPS), tiles, atoms), jnp.float32),
        pltpu.VMEM((tiles, len(STEPS), atoms, atoms), jnp.float32),
        pltpu.VMEM((tiles, 2, atoms, atoms), jnp.float32),
        pltpu.VMEM(width + (2, atoms), jnp.float32),
        pltpu.VMEM(width + (2, atoms), jnp.float32),
        pltpu.VMEM(width + (2, atoms), jnp.float32),
        pltpu.VMEM(cells + (2, atoms), jnp.float32),
    ]
    scratch += [pltpu.VMEM((ITERS, count, 2, atoms), jnp.float32) for count in group_sizes]
    scratch += [
        pltpu.SemaphoreType.DMA((6,)),
        pltpu.SemaphoreType.DMA((ITERS, KINDS)),
        pltpu.SemaphoreType.DMA((ITERS, KINDS)),
        pltpu.SemaphoreType.DMA((ITERS, len(groups))),
        pltpu.SemaphoreType.DMA((ITERS, len(groups))),
        pltpu.SemaphoreType.REGULAR((2,)),
    ]
    return kernel, scratch


def put_out(charge_in, resid_in, charge_ref, resid_ref, sems):
    copies = [
        pltpu.make_async_copy(charge_in, charge_ref, sems.at[0]),
        pltpu.make_async_copy(resid_in, resid_ref, sems.at[1]),
    ]
    for copy in copies:
        copy.start()
    for copy in copies:
        copy.wait()


def solution(mesh):
    sizes = {a: mesh.shape[a] for a in AXES}
    devices = sizes["gx"] * sizes["gy"] * sizes["gz"]
    groups = (AXES,) if devices <= 64 else tuple((a,) for a in AXES)

    def per_device(offsets, type_ids, neighbours, type_chi, type_eta, type_gamma):
        cells = offsets.shape[1:4]
        atoms = offsets.shape[4]
        types = type_chi.shape[0]
        kernel, scratch = make_kernel(sizes, groups, cells, atoms, types, 128)
        scratch[2] = pltpu.VMEM(neighbours.shape, jnp.int32)
        vmem = pl.BlockSpec(memory_space=pltpu.VMEM)
        hbm = pl.BlockSpec(memory_space=pltpu.HBM)
        pair = pl.pallas_call(
            kernel,
            out_shape=(
                jax.ShapeDtypeStruct(cells + (atoms,), jnp.float32),
                jax.ShapeDtypeStruct((2,) + cells + (atoms,), jnp.float32),
            ),
            in_specs=[hbm] * 6,
            out_specs=(vmem, vmem),
            scratch_shapes=scratch,
            compiler_params=pltpu.CompilerParams(
                collective_id=0, has_side_effects=True, vmem_limit_bytes=48 * 1024 * 1024
            ),
        )(*[pltpu.with_memory_space_constraint(v, pltpu.HBM) for v in (offsets, type_ids, neighbours, type_chi, type_eta, type_gamma)])
        return pl.pallas_call(
            put_out,
            out_shape=tuple(jax.ShapeDtypeStruct(v.shape, v.dtype) for v in pair),
            in_specs=[vmem] * 2,
            out_specs=(hbm, hbm),
            scratch_shapes=[pltpu.SemaphoreType.DMA((2,))],
        )(*[pltpu.with_memory_space_constraint(v, pltpu.VMEM) for v in pair])

    placed = (
        P(None, "gx", "gy", "gz", None),
        P("gx", "gy", "gz", None),
        P("gx", "gy", "gz", None),
        P(),
        P(),
        P(),
    )
    return jax.shard_map(
        per_device,
        mesh=mesh,
        in_specs=placed,
        out_specs=(P("gx", "gy", "gz", None), P(None, "gx", "gy", "gz", None)),
        check_vma=False,
    )
```

```python
import itertools

import jax
import jax.numpy as jnp
from jax import lax
from jax.experimental import pallas as pl
from jax.experimental.pallas import tpu as pltpu
from jax.sharding import PartitionSpec as P

ITERS = 3
CELL_EDGE = 11.0
CUTOFF = 10.0
COULOMB = 14.4
AXES = ("gx", "gy", "gz")
FAR = 1000.0
MESH = pl.DeviceIdType.MESH
STEPS = [d for d in itertools.product((-1, 0, 1), repeat=3)]
REMOTE = sorted((d for d in STEPS if d != (0, 0, 0)), key=lambda d: (-abs(d[2]), -abs(d[0])))


def make_kernel(sizes, groups, cells, atoms, types, rows):
    width = tuple(c + 2 for c in cells)
    tiles = cells[0] * cells[1] * cells[2]
    local = list(itertools.product(*[range(c) for c in cells]))
    padded = list(itertools.product(*[range(w) for w in width]))
    own = (slice(1, 1 + cells[0]), slice(0, cells[1]), slice(1, 1 + cells[2]))
    joined = sizes["gy"] == 2 and cells[1] == 2
    steps = [d for d in REMOTE if not (joined and d[1] < 0)]
    distant = [d for d in steps if d[2]]
    close = [d for d in steps if not d[2]]

    def slot(place):
        return (place[0], (place[1] - 1) % width[1], place[2])

    def rounded_sides(step):
        source, target = [], []
        for axis, (d, c) in enumerate(zip(step, cells)):
            first, low, high = (0, c + 1, c) if axis == 1 else (1, 0, c + 1)
            if d == 0:
                source.append(pl.ds(first, c))
                target.append(pl.ds(first, c))
            elif axis == 1 and joined:
                source.append(pl.ds(0, 2))
                target.append(pl.ds(2, 2))
            elif d > 0:
                source.append(pl.ds(first + c - 1, 1))
                target.append(pl.ds(low, 1))
            else:
                source.append(pl.ds(first, 1))
                target.append(pl.ds(high, 1))
        return tuple(source), tuple(target)

    group_sizes = []
    for axes in groups:
        count = 1
        for a in axes:
            count = count * sizes[a]
        group_sizes.append(count)
    paired = cells[0] == 1 and sizes["gx"] % 2 == 0
    planes = paired and len(groups) == 1
    base = atoms // (2 * tiles)
    partner_tiles = cells[1] * cells[2] if paired else 0
    plane_tiles = width[0] * width[1] * cells[2] - tiles
    side_tiles = width[0] * width[1]
    brought = [partner_tiles, plane_tiles - partner_tiles, side_tiles, side_tiles]
    brought += [plane_tiles, side_tiles, side_tiles] * (ITERS - 1)
    depth = [4] + [2] * (ITERS - 1)
    sent = sum(depth) * (plane_tiles + 2 * side_tiles) + ITERS * sum(n - 1 for n in group_sizes)

    def linear(place):
        return (place[0] * width[1] + place[1]) * width[2] + place[2]

    def inside(place, axes):
        return all(1 <= place[a] <= cells[a] for a in axes)

    def reach(place):
        if inside(place, (0, 1, 2)):
            return 0
        if not inside(place, (2,)):
            return 3
        return 1 if paired and inside(place, (1,)) and place[0] == 0 else 2

    def kernel(*refs):
        hbm, (charge_ref, resid_ref) = refs[:6], refs[6:8]
        (off_ref, type_ref, list_ref, chi_ref, eta_ref, gamma_ref) = refs[8:14]
        (fields, geometry, shields, columns, listed, blocks, sums, source) = refs[14:22]
        (first, second, own_image) = refs[22:25]
        parts = refs[25 : 25 + len(groups)]
        load_sem, send_sem, halo_recv, sum_recv, met, gauge = refs[25 + len(groups) :]

        loads = [
            pltpu.make_async_copy(a, b, load_sem.at[k])
            for k, (a, b) in enumerate(
                zip(hbm, (off_ref, type_ref, list_ref, chi_ref, eta_ref, gamma_ref))
            )
        ]
        me = {a: lax.axis_index(a) for a in AXES}
        side = 2 * (1 - lax.rem(me["gx"], 2)) if paired else 0

        def real(place):
            if paired and inside(place, (1, 2)) and place[0] != 1:
                return (side if place[0] == 0 else 2 - side,) + place[1:]
            return place

        upward = jnp.where(me["gz"] == sizes["gz"] - 1, 1, 0)
        downward = jnp.where(me["gz"] == 1, 0, 1)
        eastward = jnp.where(side == 2, 0, 1)
        westward = jnp.where(side == 2, 1, 0)

        def arrival(step, stage):
            start = 4 + 3 * (stage - 1) if stage else 1
            if step[2]:
                return start + 1 + (upward if step[2] > 0 else downward)
            if stage or not paired or step[1]:
                return start
            return eastward if step[0] > 0 else westward

        pairs = [[] for _ in range(5)]
        for t, home in enumerate(local):
            split = [[], [], []]
            for step in STEPS:
                marked = tuple(h + 1 + d for h, d in zip(home, step))
                if reach(marked) == 3:
                    continue
                place = real(marked)
                n = ((place[0] - home[0]) * 3 + step[1] + 1) * 3 + step[2] + 1
                split[reach(marked)].append((n, place, step == (0, 0, 0)))
            for kept, part in zip(pairs, split):
                kept.append((t, part))
        edge = me["gz"] == 0
        far = (jnp.where(edge, cells[2] + 1, 0), jnp.where(edge, 0, cells[2] + 1))
        for which, pz in zip((3, 4), far):
            tz = jnp.where(pz == 0, 0, cells[2] - 1)
            for x, y in itertools.product(range(cells[0]), range(cells[1])):
                part = [
                    ((a * 3 + b) * 3 + pz - tz, (x + a, y + b, pz), False)
                    for a, b in itertools.product(range(3), repeat=2)
                ]
                pairs[which].append(((x * cells[1] + y) * cells[2] + tz, part))

        def places_of(which):
            if which < 3:
                return [real(p) for p in padded if reach(p) == which]
            return [p + (far[which - 3],) for p in itertools.product(*map(range, width[:2]))]

        turned = {
            a: [lax.rem(me[a] + d, sizes[a]) if d else me[a] for d in range(sizes[a])] for a in AXES
        }

        def neighbour(step):
            return tuple(turned[a][d % sizes[a]] for a, d in zip(AXES, step))

        def member(axes, hop):
            place = dict(me)
            for a in reversed(axes):
                place[a] = turned[a][hop % sizes[a]]
                hop = hop // sizes[a]
            return tuple(place[a] for a in AXES)

        def lookup(kinds, table):
            result = jnp.zeros(kinds.shape, jnp.float32)
            for k in range(types):
                result = jnp.where(kinds == float(k), table[k], result)
            return result

        for load in loads[:2]:
            load.start()
        barrier = pltpu.get_barrier_semaphore()

        def greet(place):
            pl.semaphore_signal(barrier, inc=1, device_id=place, device_id_type=MESH)

        odd = lax.rem(me["gx"], 2)
        greeted = 0
        if planes:
            for dz in range(sizes["gz"]):
                for k, dy in itertools.product(range(sizes["gx"] // 2), range(sizes["gy"])):
                    x = me["gx"] - odd + 2 * k + (1 if dz else 0)
                    place = (
                        lax.rem(x, sizes["gx"]),
                        lax.rem(me["gy"] + dy, sizes["gy"]),
                        lax.rem(me["gz"] + dz, sizes["gz"]),
                    )
                    if (dz, k, dy) == (0, 0, 0):
                        pl.when(odd == 1)(lambda place=place: greet(place))
                    else:
                        greet(place)
        else:
            for axes, count in zip(groups, group_sizes):
                for hop in range(1, count):
                    greet(member(axes, hop))
                    greeted += 1
            if len(groups) > 1:
                for step in REMOTE:
                    greet(neighbour(step))
                    greeted += 1

        def tell(which):
            partner = (me["gx"] + 1 - 2 * odd, me["gy"], me["gz"])
            pl.semaphore_signal(met.at[which], inc=1, device_id=partner, device_id_type=MESH)

        def plane_is_in():
            @pl.when(odd == 0)
            def _():
                pl.semaphore_wait(barrier, sizes["gx"] * sizes["gy"] - 1)
                tell(0)

            @pl.when(odd == 1)
            def _():
                pl.semaphore_wait(met.at[0], 1)

        def others_are_in():
            @pl.when(odd == 1)
            def _():
                pl.semaphore_wait(barrier, sizes["gx"] * sizes["gy"] * (sizes["gz"] - 1))
                tell(1)

            @pl.when(odd == 0)
            def _():
                pl.semaphore_wait(met.at[1], 1)

        for load in loads[2:]:
            load.start()
        for load in loads[:2]:
            load.wait()

        row4 = lax.broadcasted_iota(jnp.int32, (4, atoms), 0)

        def shifted(place):
            ends = [
                CELL_EDGE * (jnp.asarray(p, jnp.int32).astype(jnp.float32) - (1.0 + 0.5 * c))
                for p, c in zip(place, cells)
            ]
            return jnp.where(row4 == 0, ends[0], jnp.where(row4 == 1, ends[1], ends[2]))

        def stacked(raw, place):
            p = jnp.where(row4 < 3, (raw + shifted(place)) * (1.0 / CUTOFF), 0.0)
            return jnp.where(row4 < 3, p, jnp.sum(p * p, axis=0, keepdims=True))

        def thirds(values):
            pieces = []
            for k in range(3):
                piece = values.astype(jnp.bfloat16).astype(jnp.float32)
                pieces.append(piece)
                if k < 2:
                    values = values - piece
            return pieces

        def sigma(kinds):
            root = lax.rsqrt(lookup(kinds, gamma_ref))
            return root * root * root * (CUTOFF**-1.5)

        for x, y, z in local:
            for f in range(3):
                fields[x + 1, y, z + 1, f : f + 1, :] = off_ref[f, x, y, z : z + 1, :]
            fields[x + 1, y, z + 1, 3:4, :] = type_ref[x, y, z : z + 1, :].astype(jnp.float32)

        def locate(places):
            for place in places:
                x, y, z = slot(place)
                kinds = fields[x, y, z, 3:4, :]
                v1, v2, v3 = thirds(stacked(fields[x, y, z], place))
                unit = jnp.where(row4 < 3, 1.0, 0.0)
                geometry[x, y, z] = jnp.concatenate(
                    [v1, v2, v3, v1, v2, v1, unit, jnp.zeros_like(unit)], axis=0
                )
                shields[x, y, z, 0:1, :] = sigma(kinds)
                source[x, y, z, 0:1, :] = -lookup(kinds, chi_ref)
                source[x, y, z, 1:2, :] = jnp.full((1, atoms), -1.0, jnp.float32)

        with jax.named_scope("barrier"):
            if planes:
                plane_is_in()
            else:
                pl.semaphore_wait(barrier, greeted)

        def halo(buffer, stage, chosen):
            for step in chosen:
                here, there = rounded_sides(step)
                pltpu.make_async_remote_copy(
                    src_ref=buffer.at[here],
                    dst_ref=buffer.at[there],
                    send_sem=send_sem.at[0],
                    recv_sem=halo_recv.at[arrival(step, stage)],
                    device_id=neighbour(step),
                    device_id_type=MESH,
                ).start()

        def all_of(count, semaphores):
            return pltpu.make_async_remote_copy(
                src_ref=gauge.at[pl.ds(0, count)],
                dst_ref=gauge.at[pl.ds(0, count)],
                send_sem=semaphores[0],
                recv_sem=semaphores[1],
                device_id=neighbour(REMOTE[0]),
                device_id_type=MESH,
            )

        def arrived(stage, which):
            index = (4 + 3 * (stage - 1) - 1 if stage else 0) + which
            all_of(
                brought[index] * depth[stage], (send_sem.at[0], halo_recv.at[index])
            ).wait_recv()

        def coupling(t, n, place, at, own_part, itself):
            x, y, z = place
            square = lax.dot_general(
                own_part[0][:, :32],
                geometry[x, y, z],
                (((1,), (0,)), ((), ())),
                preferred_element_type=jnp.float32,
            )
            if itself:
                i = lax.broadcasted_iota(jnp.int32, (rows, atoms), 0) + at
                j = lax.broadcasted_iota(jnp.int32, (rows, atoms), 1)
                square = jnp.where(i == j, 4.0, square)
            u = square * lax.rsqrt(square)
            w = jnp.maximum(listed[n, pl.ds(t, 1), :] - u, 0.0)
            w = w * w
            w = w * w
            shape = (u + 0.5) * (square + 0.2) - 0.05
            cube = square * u + own_part[1] * shields[x, y, z, 0:1, :]
            return w * shape * jnp.exp2(jnp.log2(cube) * (-1.0 / 3.0))

        lanes = lax.broadcasted_iota(jnp.int32, (rows, atoms), 1)

        def fold(first_half, second_half, shift):
            clear = (lanes & shift) == 0
            kept = jnp.where(clear, first_half, second_half)
            return kept + pltpu.roll(jnp.where(clear, second_half, first_half), shift, 1)

        def tile_pass(vector, groups_now, building):
            merged = [(t, list(part)) for t, part in pairs[groups_now[0]]]
            for which in groups_now[1:]:
                for (_, kept), (_, part) in zip(merged, pairs[which]):
                    kept.extend(part)

            def slab(index, carry):
                at = pl.multiple_of(index * rows, rows)
                for t, part in merged:
                    if 0 in groups_now:
                        total_s = jnp.zeros((rows, atoms), jnp.float32)
                        total_t = jnp.zeros((rows, atoms), jnp.float32)
                    else:
                        total_s = sums[t, 0, pl.ds(at, rows), :]
                        total_t = sums[t, 1, pl.ds(at, rows), :]
                    if building:
                        own_part = [columns[t, f, pl.ds(at, rows), :] for f in range(2)]
                    for n, place, itself in part:
                        x, y, z = slot(place)
                        if building:
                            block = coupling(t, n, (x, y, z), at, own_part, itself)
                            blocks[t, n, pl.ds(at, rows), :] = block
                            total_t = total_t - block
                        else:
                            block = blocks[t, n, pl.ds(at, rows), :]
                            total_t = total_t + block * vector[x, y, z, 1:2, :]
                        total_s = total_s + block * vector[x, y, z, 0:1, :]
                    sums[t, 0, pl.ds(at, rows), :] = total_s
                    sums[t, 1, pl.ds(at, rows), :] = total_t
                return carry

            lax.fori_loop(0, atoms // rows, slab, 0)

        scale = 20.0 * COULOMB / CUTOFF
        high = max(16, 2 * tiles)
        sheaf = lax.broadcasted_iota(jnp.int32, (high, 3 * atoms), 1) % atoms // base
        gather = jnp.where(
            sheaf == lax.broadcasted_iota(jnp.int32, (high, 3 * atoms), 0), 1.0, 0.0
        ).astype(jnp.bfloat16)

        def collect(vector, image):
            folded = []
            for at in range(0, atoms, rows):
                left = [sums[t, k, at : at + rows, :] for t in range(tiles) for k in range(2)]
                shift = base
                while len(left) > 1:
                    left = [fold(a, b, shift) for a, b in zip(left[::2], left[1::2])]
                    shift = 2 * shift
                folded.append(left[0])
            left = jnp.concatenate(folded, axis=0)
            pieces = []
            for k in range(3):
                piece = left.astype(jnp.bfloat16)
                pieces.append(piece)
                if k < 2:
                    left = left - piece.astype(jnp.float32)
            result = lax.dot_general(
                gather,
                jnp.concatenate(pieces, axis=1),
                (((1,), (1,)), ((), ())),
                preferred_element_type=jnp.float32,
            )
            for t, (x, y, z) in enumerate(local):
                here = vector[x + 1, y, z + 1]
                image(x, y, z, eta[t] * here + scale * result[2 * t : 2 * t + 2])

        def to_padded(buffer):
            def store(x, y, z, pair):
                buffer[x + 1, y, z + 1] = pair

            return store

        def to_own(x, y, z, pair):
            own_image[x, y, z] = pair

        lane = lax.broadcasted_iota(jnp.int32, (1, atoms), 1)
        half = atoms // 2

        def over_own(values):
            return jnp.sum(jnp.sum(values, axis=(0, 1, 2)), axis=1, keepdims=True)

        def sum_copies(g, stage):
            axes, count = groups[g], group_sizes[g]
            return [
                pltpu.make_async_remote_copy(
                    src_ref=parts[g].at[stage, 0],
                    dst_ref=parts[g].at[stage, hop],
                    send_sem=send_sem.at[0],
                    recv_sem=sum_recv.at[stage, g],
                    device_id=member(axes, hop),
                    device_id_type=MESH,
                )
                for hop in range(1, count)
            ]

        def start_sums(values, stage):
            message = jnp.zeros((1, atoms), jnp.float32)
            for k, value in enumerate(values):
                for row in range(2):
                    message = jnp.where(lane == k + row * half, value[row : row + 1], message)
            parts[0][stage, 0] = message
            for copy in sum_copies(0, stage):
                copy.start()

        def finish_sums(number, stage):
            for g in range(len(groups)):
                all_of(group_sizes[g] - 1, (send_sem.at[0], sum_recv.at[stage, g])).wait_recv()
                total = jnp.sum(parts[g][stage], axis=0)
                if g + 1 < len(groups):
                    parts[g + 1][stage, 0] = total
                    for copy in sum_copies(g + 1, stage):
                        copy.start()
            def picked(k):
                return jnp.sum(jnp.where(lane == k, total, 0.0), axis=1, keepdims=True)

            first_row = lax.broadcasted_iota(jnp.int32, (2, 1), 0) == 0
            return [jnp.where(first_row, picked(k), picked(k + half)) for k in range(number)]

        def distant_positions():
            others_are_in()
            halo(fields, 0, distant)

        last = me["gz"] == sizes["gz"] - 1
        if planes:
            halo(fields, 0, close)
            pl.when(last)(distant_positions)
        else:
            halo(fields, 0, steps)
        for load in loads[2:]:
            load.wait()
        locate(places_of(0))
        for t, (x, y, z) in enumerate(local):
            place = (x + 1, y + 1, z + 1)
            v1, v2, v3 = thirds(stacked(fields[slot(place)], place))
            c1 = jnp.where(row4 < 3, -2.0 * v1, 1.0)
            c2 = jnp.where(row4 < 3, -2.0 * v2, 0.0)
            c3 = jnp.where(row4 < 3, -2.0 * v3, 0.0)
            norms = jnp.where(
                row4 == 0, v1[3:4], jnp.where(row4 == 1, v2[3:4], jnp.where(row4 == 2, v3[3:4], 0.0))
            )
            none = jnp.zeros((atoms - 28, atoms), jnp.float32)
            columns[t, 0] = jnp.transpose(
                jnp.concatenate([c1, c1, c1, c2, c2, c3, norms, none], axis=0)
            )
            row = shields[x + 1, y, z + 1, 0:1, :]
            columns[t, 1] = jnp.transpose(jnp.broadcast_to(row, (atoms, atoms)))
        entries = jnp.concatenate(
            [list_ref[x, y, z : z + 1, :] - linear((x + 1, y + 1, z + 1)) for x, y, z in local], 0
        )
        for n, step in enumerate(STEPS):
            found = jnp.max(
                jnp.where(entries == linear(step), 1.0, 0.0), axis=1, keepdims=True
            )
            listed[n] = jnp.broadcast_to(1.0 - (1.0 - found) * FAR, (tiles, atoms))
        eta = [lookup(fields[x + 1, y, z + 1, 3:4, :], eta_ref) for x, y, z in local]

        with jax.named_scope("build0"):
            tile_pass(source, (0,), True)
        for which in (1, 2, 3, 4) if paired else (2, 3, 4):
            if which == 2 and planes:
                with jax.named_scope("others"):
                    pl.when(jnp.logical_not(last))(distant_positions)
            with jax.named_scope(f"wait_pos{which}"):
                arrived(0, which - 1)
            locate(places_of(which))
            with jax.named_scope(f"build{which}"):
                tile_pass(source, (which,), True)
        with jax.named_scope("collect0"):
            collect(source, to_padded(first))

        def apply(vector, stage, number):
            with jax.named_scope(f"pass{stage}_0"):
                tile_pass(vector, (0,), False)
            with jax.named_scope(f"wait{stage}_1"):
                arrived(stage, 1)
            with jax.named_scope(f"pass{stage}_1"):
                tile_pass(vector, (1, 2) if paired else (2,), False)
            for which in (3, 4):
                with jax.named_scope(f"wait{stage}_{which}"):
                    arrived(stage, which - 1)
                with jax.named_scope(f"pass{stage}_{which}"):
                    tile_pass(vector, (which,), False)
            with jax.named_scope(f"collect{stage}"):
                collect(vector, to_own)
            with jax.named_scope(f"sums{stage}"):
                return finish_sums(number, stage - 1)

        residual = source[own]
        image = first[own]
        values = [over_own(residual * residual), over_own(residual * image)]
        halo(first, 1, distant)
        start_sums(values, 0)
        halo(first, 1, close)
        norm_now, curvature = apply(first, 1, 2)
        step_size = norm_now / curvature
        closing = 1.0 / (norm_now * step_size)
        direction, along = residual, image
        further = own_image[...]
        answer = step_size * direction
        residual = residual - step_size * along
        image = image - step_size * further
        second[own] = image
        values = [over_own(residual * residual), over_own(residual * image)]
        halo(second, 2, distant)
        start_sums(values, 1)
        halo(second, 2, close)
        norm_next, curvature = apply(second, 2, 2)
        growth = norm_next / norm_now
        step_size = norm_next / (curvature - norm_next * norm_next * closing)
        closing = 1.0 / (norm_next * step_size)
        norm_now = norm_next
        further = own_image[...] + growth * further
        direction = residual + growth * direction
        along = image + growth * along
        answer = answer + step_size * direction
        residual = residual - step_size * along
        image = image - step_size * further
        values = [residual * residual, residual * image, answer, residual, direction]
        start_sums([over_own(v) for v in values], 2)
        with jax.named_scope("sums2"):
            norm_next, curvature, *others = finish_sums(5, 2)
        growth = norm_next / norm_now
        step_size = norm_next / (curvature - norm_next * norm_next * closing)
        answer = answer + step_size * (residual + growth * direction)
        residual = residual - step_size * (image + growth * along)
        totals = others[0] + step_size * (others[1] + growth * others[2])
        level = totals[0:1] / totals[1:2]
        for x, y, z in local:
            charge_ref[x, y, z : z + 1, :] = 1000.0 * (
                answer[x, y, z, 0:1] - level * answer[x, y, z, 1:2]
            )
            for s in range(2):
                resid_ref[s, x, y, z : z + 1, :] = residual[x, y, z, s : s + 1]
        with jax.named_scope("drain"):
            all_of(sent, (send_sem.at[0], halo_recv.at[0])).wait_send()

    scratch = [
        pltpu.VMEM((3,) + cells + (atoms,), jnp.float32),
        pltpu.VMEM(cells + (atoms,), jnp.int32),
        None,
        pltpu.SMEM((types,), jnp.float32),
        pltpu.SMEM((types,), jnp.float32),
        pltpu.SMEM((types,), jnp.float32),
        pltpu.VMEM(width + (4, atoms), jnp.float32),
        pltpu.VMEM(width + (32, atoms), jnp.float32),
        pltpu.VMEM(width + (1, atoms), jnp.float32),
        pltpu.VMEM((tiles, 2, atoms, atoms), jnp.float32),
        pltpu.VMEM((len(STEPS), tiles, atoms), jnp.float32),
        pltpu.VMEM((tiles, len(STEPS), atoms, atoms), jnp.float32),
        pltpu.VMEM((tiles, 2, atoms, atoms), jnp.float32),
        pltpu.VMEM(width + (2, atoms), jnp.float32),
        pltpu.VMEM(width + (2, atoms), jnp.float32),
        pltpu.VMEM(width + (2, atoms), jnp.float32),
        pltpu.VMEM(cells + (2, atoms), jnp.float32),
    ]
    scratch += [pltpu.VMEM((ITERS, count, 1, atoms), jnp.float32) for count in group_sizes]
    scratch += [
        pltpu.SemaphoreType.DMA((6,)),
        pltpu.SemaphoreType.DMA((1,)),
        pltpu.SemaphoreType.DMA((len(brought),)),
        pltpu.SemaphoreType.DMA((ITERS, len(groups))),
        pltpu.SemaphoreType.REGULAR((2,)),
        pltpu.VMEM((sent, 1, atoms), jnp.float32),
    ]
    return kernel, scratch


def put_out(charge_in, resid_in, charge_ref, resid_ref, sems):
    copies = [
        pltpu.make_async_copy(charge_in, charge_ref, sems.at[0]),
        pltpu.make_async_copy(resid_in, resid_ref, sems.at[1]),
    ]
    for copy in copies:
        copy.start()
    for copy in copies:
        copy.wait()


def solution(mesh):
    sizes = {a: mesh.shape[a] for a in AXES}
    devices = sizes["gx"] * sizes["gy"] * sizes["gz"]
    groups = (AXES,) if devices <= 64 else tuple((a,) for a in AXES)

    def per_device(offsets, type_ids, neighbours, type_chi, type_eta, type_gamma):
        cells = offsets.shape[1:4]
        atoms = offsets.shape[4]
        types = type_chi.shape[0]
        kernel, scratch = make_kernel(sizes, groups, cells, atoms, types, 128)
        scratch[2] = pltpu.VMEM(neighbours.shape, jnp.int32)
        vmem = pl.BlockSpec(memory_space=pltpu.VMEM)
        hbm = pl.BlockSpec(memory_space=pltpu.HBM)
        pair = pl.pallas_call(
            kernel,
            out_shape=(
                jax.ShapeDtypeStruct(cells + (atoms,), jnp.float32),
                jax.ShapeDtypeStruct((2,) + cells + (atoms,), jnp.float32),
            ),
            in_specs=[hbm] * 6,
            out_specs=(vmem, vmem),
            scratch_shapes=scratch,
            compiler_params=pltpu.CompilerParams(
                collective_id=0, has_side_effects=True, vmem_limit_bytes=48 * 1024 * 1024
            ),
        )(*[pltpu.with_memory_space_constraint(v, pltpu.HBM) for v in (offsets, type_ids, neighbours, type_chi, type_eta, type_gamma)])
        return pl.pallas_call(
            put_out,
            out_shape=tuple(jax.ShapeDtypeStruct(v.shape, v.dtype) for v in pair),
            in_specs=[vmem] * 2,
            out_specs=(hbm, hbm),
            scratch_shapes=[pltpu.SemaphoreType.DMA((2,))],
        )(*[pltpu.with_memory_space_constraint(v, pltpu.VMEM) for v in pair])

    placed = (
        P(None, "gx", "gy", "gz", None),
        P("gx", "gy", "gz", None),
        P("gx", "gy", "gz", None),
        P(),
        P(),
        P(),
    )
    return jax.shard_map(
        per_device,
        mesh=mesh,
        in_specs=placed,
        out_specs=(P("gx", "gy", "gz", None), P(None, "gx", "gy", "gz", None)),
        check_vma=False,
    )
```

```python
import itertools

import jax
import jax.numpy as jnp
from jax import lax
from jax.experimental import pallas as pl
from jax.experimental.pallas import tpu as pltpu
from jax.sharding import PartitionSpec as P

ITERS = 3
CELL_EDGE = 11.0
CUTOFF = 10.0
COULOMB = 14.4
AXES = ("gx", "gy", "gz")
FAR = 1000.0
MESH = pl.DeviceIdType.MESH
STEPS = [d for d in itertools.product((-1, 0, 1), repeat=3)]
REMOTE = sorted((d for d in STEPS if d != (0, 0, 0)), key=lambda d: (-abs(d[2]), -abs(d[0])))


def make_kernel(sizes, groups, cells, atoms, types, rows):
    width = tuple(c + 2 for c in cells)
    tiles = cells[0] * cells[1] * cells[2]
    local = list(itertools.product(*[range(c) for c in cells]))
    padded = list(itertools.product(*[range(w) for w in width]))
    own = (slice(1, 1 + cells[0]), slice(0, cells[1]), slice(1, 1 + cells[2]))
    joined = sizes["gy"] == 2 and cells[1] == 2
    steps = [d for d in REMOTE if not (joined and d[1] < 0)]
    distant = [d for d in steps if d[2]]
    close = [d for d in steps if not d[2]]

    def slot(place):
        return (place[0], (place[1] - 1) % width[1], place[2])

    def rounded_sides(step):
        source, target = [], []
        for axis, (d, c) in enumerate(zip(step, cells)):
            first, low, high = (0, c + 1, c) if axis == 1 else (1, 0, c + 1)
            if d == 0:
                source.append(pl.ds(first, c))
                target.append(pl.ds(first, c))
            elif axis == 1 and joined:
                source.append(pl.ds(0, 2))
                target.append(pl.ds(2, 2))
            elif d > 0:
                source.append(pl.ds(first + c - 1, 1))
                target.append(pl.ds(low, 1))
            else:
                source.append(pl.ds(first, 1))
                target.append(pl.ds(high, 1))
        return tuple(source), tuple(target)

    group_sizes = []
    for axes in groups:
        count = 1
        for a in axes:
            count = count * sizes[a]
        group_sizes.append(count)
    paired = cells[0] == 1 and sizes["gx"] % 2 == 0
    planes = paired and len(groups) == 1
    base = atoms // (2 * tiles)
    partner_tiles = cells[1] * cells[2] if paired else 0
    plane_tiles = width[0] * width[1] * cells[2] - tiles
    side_tiles = width[0] * width[1]
    brought = [partner_tiles, plane_tiles - partner_tiles, side_tiles, side_tiles]
    brought += [plane_tiles, side_tiles, side_tiles] * (ITERS - 1)
    depth = [4] + [2] * (ITERS - 1)
    sent = sum(depth) * (plane_tiles + 2 * side_tiles) + ITERS * sum(n - 1 for n in group_sizes)

    def linear(place):
        return (place[0] * width[1] + place[1]) * width[2] + place[2]

    def inside(place, axes):
        return all(1 <= place[a] <= cells[a] for a in axes)

    def reach(place):
        if inside(place, (0, 1, 2)):
            return 0
        if not inside(place, (2,)):
            return 3
        return 1 if paired and inside(place, (1,)) and place[0] == 0 else 2

    def kernel(*refs):
        hbm, (charge_ref, resid_ref) = refs[:6], refs[6:8]
        (off_ref, type_ref, list_ref, chi_ref, eta_ref, gamma_ref) = refs[8:14]
        (fields, geometry, shields, columns, listed, blocks, sums, source) = refs[14:22]
        (first, second, own_image) = refs[22:25]
        parts = refs[25 : 25 + len(groups)]
        load_sem, send_sem, halo_recv, sum_recv, met, gauge = refs[25 + len(groups) :]

        loads = [
            pltpu.make_async_copy(a, b, load_sem.at[k])
            for k, (a, b) in enumerate(
                zip(hbm, (off_ref, type_ref, list_ref, chi_ref, eta_ref, gamma_ref))
            )
        ]
        me = {a: lax.axis_index(a) for a in AXES}
        side = 2 * (1 - lax.rem(me["gx"], 2)) if paired else 0

        def real(place):
            if paired and inside(place, (1, 2)) and place[0] != 1:
                return (side if place[0] == 0 else 2 - side,) + place[1:]
            return place

        upward = jnp.where(me["gz"] == sizes["gz"] - 1, 1, 0)
        downward = jnp.where(me["gz"] == 1, 0, 1)
        eastward = jnp.where(side == 2, 0, 1)
        westward = jnp.where(side == 2, 1, 0)

        def arrival(step, stage):
            start = 4 + 3 * (stage - 1) if stage else 1
            if step[2]:
                return start + 1 + (upward if step[2] > 0 else downward)
            if stage or not paired or step[1]:
                return start
            return eastward if step[0] > 0 else westward

        pairs = [[] for _ in range(5)]
        for t, home in enumerate(local):
            split = [[], [], []]
            for step in STEPS:
                marked = tuple(h + 1 + d for h, d in zip(home, step))
                if reach(marked) == 3:
                    continue
                place = real(marked)
                n = ((place[0] - home[0]) * 3 + step[1] + 1) * 3 + step[2] + 1
                split[reach(marked)].append((n, place, step == (0, 0, 0)))
            for kept, part in zip(pairs, split):
                kept.append((t, part))
        edge = me["gz"] == 0
        far = (jnp.where(edge, cells[2] + 1, 0), jnp.where(edge, 0, cells[2] + 1))
        for which, pz in zip((3, 4), far):
            tz = jnp.where(pz == 0, 0, cells[2] - 1)
            for x, y in itertools.product(range(cells[0]), range(cells[1])):
                part = [
                    ((a * 3 + b) * 3 + pz - tz, (x + a, y + b, pz), False)
                    for a, b in itertools.product(range(3), repeat=2)
                ]
                pairs[which].append(((x * cells[1] + y) * cells[2] + tz, part))

        def places_of(which):
            if which < 3:
                return [real(p) for p in padded if reach(p) == which]
            return [p + (far[which - 3],) for p in itertools.product(*map(range, width[:2]))]

        turned = {
            a: [lax.rem(me[a] + d, sizes[a]) if d else me[a] for d in range(sizes[a])] for a in AXES
        }

        def neighbour(step):
            return tuple(turned[a][d % sizes[a]] for a, d in zip(AXES, step))

        def member(axes, hop):
            place = dict(me)
            for a in reversed(axes):
                place[a] = turned[a][hop % sizes[a]]
                hop = hop // sizes[a]
            return tuple(place[a] for a in AXES)

        def lookup(kinds, table):
            result = jnp.zeros(kinds.shape, jnp.float32)
            for k in range(types):
                result = jnp.where(kinds == float(k), table[k], result)
            return result

        for load in loads[:2]:
            load.start()
        barrier = pltpu.get_barrier_semaphore()

        def greet(place):
            pl.semaphore_signal(barrier, inc=1, device_id=place, device_id_type=MESH)

        odd = lax.rem(me["gx"], 2)
        greeted = 0
        if planes:
            for dz in range(sizes["gz"]):
                for k, dy in itertools.product(range(sizes["gx"] // 2), range(sizes["gy"])):
                    x = me["gx"] - odd + 2 * k + (1 if dz else 0)
                    place = (
                        lax.rem(x, sizes["gx"]),
                        lax.rem(me["gy"] + dy, sizes["gy"]),
                        lax.rem(me["gz"] + dz, sizes["gz"]),
                    )
                    if (dz, k, dy) == (0, 0, 0):
                        pl.when(odd == 1)(lambda place=place: greet(place))
                    else:
                        greet(place)
        else:
            for axes, count in zip(groups, group_sizes):
                for hop in range(1, count):
                    greet(member(axes, hop))
                    greeted += 1
            if len(groups) > 1:
                for step in REMOTE:
                    greet(neighbour(step))
                    greeted += 1

        def tell(which):
            partner = (me["gx"] + 1 - 2 * odd, me["gy"], me["gz"])
            pl.semaphore_signal(met.at[which], inc=1, device_id=partner, device_id_type=MESH)

        def plane_is_in():
            @pl.when(odd == 0)
            def _():
                pl.semaphore_wait(barrier, sizes["gx"] * sizes["gy"] - 1)
                tell(0)

            @pl.when(odd == 1)
            def _():
                pl.semaphore_wait(met.at[0], 1)

        def others_are_in():
            @pl.when(odd == 1)
            def _():
                pl.semaphore_wait(barrier, sizes["gx"] * sizes["gy"] * (sizes["gz"] - 1))
                tell(1)

            @pl.when(odd == 0)
            def _():
                pl.semaphore_wait(met.at[1], 1)

        for load in loads[2:]:
            load.start()
        with jax.named_scope("barrier"):
            if planes:
                plane_is_in()
            else:
                pl.semaphore_wait(barrier, greeted)

        for load in loads[:2]:
            load.wait()

        row4 = lax.broadcasted_iota(jnp.int32, (4, atoms), 0)

        def shifted(place):
            ends = [
                CELL_EDGE * (jnp.asarray(p, jnp.int32).astype(jnp.float32) - (1.0 + 0.5 * c))
                for p, c in zip(place, cells)
            ]
            return jnp.where(row4 == 0, ends[0], jnp.where(row4 == 1, ends[1], ends[2]))

        def stacked(raw, place):
            p = jnp.where(row4 < 3, (raw + shifted(place)) * (1.0 / CUTOFF), 0.0)
            return jnp.where(row4 < 3, p, jnp.sum(p * p, axis=0, keepdims=True))

        def thirds(values):
            pieces = []
            for k in range(3):
                piece = values.astype(jnp.bfloat16).astype(jnp.float32)
                pieces.append(piece)
                if k < 2:
                    values = values - piece
            return pieces

        def sigma(kinds):
            root = lax.rsqrt(lookup(kinds, gamma_ref))
            return root * root * root * (CUTOFF**-1.5)

        for x, y, z in local:
            for f in range(3):
                fields[x + 1, y, z + 1, f : f + 1, :] = off_ref[f, x, y, z : z + 1, :]
            fields[x + 1, y, z + 1, 3:4, :] = type_ref[x, y, z : z + 1, :].astype(jnp.float32)

        def locate(places):
            for place in places:
                x, y, z = slot(place)
                kinds = fields[x, y, z, 3:4, :]
                v1, v2, v3 = thirds(stacked(fields[x, y, z], place))
                unit = jnp.where(row4 < 3, 1.0, 0.0)
                geometry[x, y, z] = jnp.concatenate(
                    [v1, v2, v3, v1, v2, v1, unit, jnp.zeros_like(unit)], axis=0
                )
                shields[x, y, z, 0:1, :] = sigma(kinds)
                source[x, y, z, 0:1, :] = -lookup(kinds, chi_ref)
                source[x, y, z, 1:2, :] = jnp.full((1, atoms), -1.0, jnp.float32)

        def halo(buffer, stage, chosen):
            for step in chosen:
                here, there = rounded_sides(step)
                pltpu.make_async_remote_copy(
                    src_ref=buffer.at[here],
                    dst_ref=buffer.at[there],
                    send_sem=send_sem.at[0],
                    recv_sem=halo_recv.at[arrival(step, stage)],
                    device_id=neighbour(step),
                    device_id_type=MESH,
                ).start()

        def all_of(count, semaphores):
            return pltpu.make_async_remote_copy(
                src_ref=gauge.at[pl.ds(0, count)],
                dst_ref=gauge.at[pl.ds(0, count)],
                send_sem=semaphores[0],
                recv_sem=semaphores[1],
                device_id=neighbour(REMOTE[0]),
                device_id_type=MESH,
            )

        def arrived(stage, which):
            index = (4 + 3 * (stage - 1) - 1 if stage else 0) + which
            all_of(
                brought[index] * depth[stage], (send_sem.at[0], halo_recv.at[index])
            ).wait_recv()

        def coupling(t, n, place, at, own_part, itself):
            x, y, z = place
            square = lax.dot_general(
                own_part[0][:, :32],
                geometry[x, y, z],
                (((1,), (0,)), ((), ())),
                preferred_element_type=jnp.float32,
            )
            if itself:
                i = lax.broadcasted_iota(jnp.int32, (rows, atoms), 0) + at
                j = lax.broadcasted_iota(jnp.int32, (rows, atoms), 1)
                square = jnp.where(i == j, 4.0, square)
            square = jnp.maximum(square, 1e-6)
            u = square * lax.rsqrt(square)
            w = jnp.maximum(listed[n, pl.ds(t, 1), :] - u, 0.0)
            w = w * w
            w = w * w
            shape = (u + 0.5) * (square + 0.2) - 0.05
            cube = square * u + own_part[1] * shields[x, y, z, 0:1, :]
            return w * shape * jnp.exp2(jnp.log2(cube) * (-1.0 / 3.0))

        lanes = lax.broadcasted_iota(jnp.int32, (rows, atoms), 1)

        def fold(first_half, second_half, shift):
            clear = (lanes & shift) == 0
            kept = jnp.where(clear, first_half, second_half)
            return kept + pltpu.roll(jnp.where(clear, second_half, first_half), shift, 1)

        def tile_pass(vector, groups_now, building):
            merged = [(t, list(part)) for t, part in pairs[groups_now[0]]]
            for which in groups_now[1:]:
                for (_, kept), (_, part) in zip(merged, pairs[which]):
                    kept.extend(part)

            def slab(index, carry):
                at = pl.multiple_of(index * rows, rows)
                for t, part in merged:
                    if 0 in groups_now:
                        total_s = jnp.zeros((rows, atoms), jnp.float32)
                        total_t = jnp.zeros((rows, atoms), jnp.float32)
                    else:
                        total_s = sums[t, 0, pl.ds(at, rows), :]
                        total_t = sums[t, 1, pl.ds(at, rows), :]
                    if building:
                        own_part = [columns[t, f, pl.ds(at, rows), :] for f in range(2)]
                    for n, place, itself in part:
                        x, y, z = slot(place)
                        if building:
                            block = coupling(t, n, (x, y, z), at, own_part, itself)
                            blocks[t, n, pl.ds(at, rows), :] = block
                            total_t = total_t - block
                        else:
                            block = blocks[t, n, pl.ds(at, rows), :]
                            total_t = total_t + block * vector[x, y, z, 1:2, :]
                        total_s = total_s + block * vector[x, y, z, 0:1, :]
                    sums[t, 0, pl.ds(at, rows), :] = total_s
                    sums[t, 1, pl.ds(at, rows), :] = total_t
                return carry

            lax.fori_loop(0, atoms // rows, slab, 0)

        scale = 20.0 * COULOMB / CUTOFF
        high = max(16, 2 * tiles)
        sheaf = lax.broadcasted_iota(jnp.int32, (high, 3 * atoms), 1) % atoms // base
        gather = jnp.where(
            sheaf == lax.broadcasted_iota(jnp.int32, (high, 3 * atoms), 0), 1.0, 0.0
        ).astype(jnp.bfloat16)

        def collect(vector, image):
            folded = []
            for at in range(0, atoms, rows):
                left = [sums[t, k, at : at + rows, :] for t in range(tiles) for k in range(2)]
                shift = base
                while len(left) > 1:
                    left = [fold(a, b, shift) for a, b in zip(left[::2], left[1::2])]
                    shift = 2 * shift
                folded.append(left[0])
            left = jnp.concatenate(folded, axis=0)
            pieces = []
            for k in range(3):
                piece = left.astype(jnp.bfloat16)
                pieces.append(piece)
                if k < 2:
                    left = left - piece.astype(jnp.float32)
            result = lax.dot_general(
                gather,
                jnp.concatenate(pieces, axis=1),
                (((1,), (1,)), ((), ())),
                preferred_element_type=jnp.float32,
            )
            for t, (x, y, z) in enumerate(local):
                here = vector[x + 1, y, z + 1]
                image(x, y, z, eta[t] * here + scale * result[2 * t : 2 * t + 2])

        def to_padded(buffer):
            def store(x, y, z, pair):
                buffer[x + 1, y, z + 1] = pair

            return store

        def to_own(x, y, z, pair):
            own_image[x, y, z] = pair

        lane = lax.broadcasted_iota(jnp.int32, (1, atoms), 1)
        half = atoms // 2

        def over_own(values):
            return jnp.sum(jnp.sum(values, axis=(0, 1, 2)), axis=1, keepdims=True)

        def sum_copies(g, stage):
            axes, count = groups[g], group_sizes[g]
            return [
                pltpu.make_async_remote_copy(
                    src_ref=parts[g].at[stage, 0],
                    dst_ref=parts[g].at[stage, hop],
                    send_sem=send_sem.at[0],
                    recv_sem=sum_recv.at[stage, g],
                    device_id=member(axes, hop),
                    device_id_type=MESH,
                )
                for hop in range(1, count)
            ]

        def start_sums(values, stage):
            message = jnp.zeros((1, atoms), jnp.float32)
            for k, value in enumerate(values):
                for row in range(2):
                    message = jnp.where(lane == k + row * half, value[row : row + 1], message)
            parts[0][stage, 0] = message
            for copy in sum_copies(0, stage):
                copy.start()

        def finish_sums(number, stage):
            for g in range(len(groups)):
                all_of(group_sizes[g] - 1, (send_sem.at[0], sum_recv.at[stage, g])).wait_recv()
                total = jnp.sum(parts[g][stage], axis=0)
                if g + 1 < len(groups):
                    parts[g + 1][stage, 0] = total
                    for copy in sum_copies(g + 1, stage):
                        copy.start()
            def picked(k):
                return jnp.sum(jnp.where(lane == k, total, 0.0), axis=1, keepdims=True)

            first_row = lax.broadcasted_iota(jnp.int32, (2, 1), 0) == 0
            return [jnp.where(first_row, picked(k), picked(k + half)) for k in range(number)]

        def distant_positions():
            others_are_in()
            halo(fields, 0, distant)

        last = me["gz"] == sizes["gz"] - 1
        if planes:
            halo(fields, 0, close)
            pl.when(last)(distant_positions)
        else:
            halo(fields, 0, steps)
        for load in loads[2:]:
            load.wait()
        locate(places_of(0))
        for t, (x, y, z) in enumerate(local):
            place = (x + 1, y + 1, z + 1)
            v1, v2, v3 = thirds(stacked(fields[slot(place)], place))
            c1 = jnp.where(row4 < 3, -2.0 * v1, 1.0)
            c2 = jnp.where(row4 < 3, -2.0 * v2, 0.0)
            c3 = jnp.where(row4 < 3, -2.0 * v3, 0.0)
            norms = jnp.where(
                row4 == 0, v1[3:4], jnp.where(row4 == 1, v2[3:4], jnp.where(row4 == 2, v3[3:4], 0.0))
            )
            none = jnp.zeros((atoms - 28, atoms), jnp.float32)
            columns[t, 0] = jnp.transpose(
                jnp.concatenate([c1, c1, c1, c2, c2, c3, norms, none], axis=0)
            )
            row = shields[x + 1, y, z + 1, 0:1, :]
            columns[t, 1] = jnp.transpose(jnp.broadcast_to(row, (atoms, atoms)))
        entries = jnp.concatenate(
            [list_ref[x, y, z : z + 1, :] - linear((x + 1, y + 1, z + 1)) for x, y, z in local], 0
        )
        for n, step in enumerate(STEPS):
            found = jnp.max(
                jnp.where(entries == linear(step), 1.0, 0.0), axis=1, keepdims=True
            )
            listed[n] = jnp.broadcast_to(1.0 - (1.0 - found) * FAR, (tiles, atoms))
        eta = [lookup(fields[x + 1, y, z + 1, 3:4, :], eta_ref) for x, y, z in local]

        with jax.named_scope("build0"):
            tile_pass(source, (0,), True)
        for which in (1, 2, 3, 4) if paired else (2, 3, 4):
            if which == 2 and planes:
                with jax.named_scope("others"):
                    pl.when(jnp.logical_not(last))(distant_positions)
            with jax.named_scope(f"wait_pos{which}"):
                arrived(0, which - 1)
            locate(places_of(which))
            with jax.named_scope(f"build{which}"):
                tile_pass(source, (which,), True)
        with jax.named_scope("collect0"):
            collect(source, to_padded(first))

        def apply(vector, stage, number):
            with jax.named_scope(f"pass{stage}_0"):
                tile_pass(vector, (0,), False)
            with jax.named_scope(f"wait{stage}_1"):
                arrived(stage, 1)
            with jax.named_scope(f"pass{stage}_1"):
                tile_pass(vector, (1, 2) if paired else (2,), False)
            for which in (3, 4):
                with jax.named_scope(f"wait{stage}_{which}"):
                    arrived(stage, which - 1)
                with jax.named_scope(f"pass{stage}_{which}"):
                    tile_pass(vector, (which,), False)
            with jax.named_scope(f"collect{stage}"):
                collect(vector, to_own)
            with jax.named_scope(f"sums{stage}"):
                return finish_sums(number, stage - 1)

        residual = source[own]
        image = first[own]
        values = [over_own(residual * residual), over_own(residual * image)]
        halo(first, 1, distant)
        halo(first, 1, close)
        start_sums(values, 0)
        norm_now, curvature = apply(first, 1, 2)
        step_size = norm_now / curvature
        closing = 1.0 / (norm_now * step_size)
        direction, along = residual, image
        further = own_image[...]
        answer = step_size * direction
        residual = residual - step_size * along
        image = image - step_size * further
        second[own] = image
        values = [over_own(residual * residual), over_own(residual * image)]
        halo(second, 2, distant)
        halo(second, 2, close)
        start_sums(values, 1)
        norm_next, curvature = apply(second, 2, 2)
        growth = norm_next / norm_now
        step_size = norm_next / (curvature - norm_next * norm_next * closing)
        closing = 1.0 / (norm_next * step_size)
        norm_now = norm_next
        further = own_image[...] + growth * further
        direction = residual + growth * direction
        along = image + growth * along
        answer = answer + step_size * direction
        residual = residual - step_size * along
        image = image - step_size * further
        values = [residual * residual, residual * image, answer, residual, direction]
        start_sums([over_own(v) for v in values], 2)
        with jax.named_scope("sums2"):
            norm_next, curvature, *others = finish_sums(5, 2)
        growth = norm_next / norm_now
        step_size = norm_next / (curvature - norm_next * norm_next * closing)
        answer = answer + step_size * (residual + growth * direction)
        residual = residual - step_size * (image + growth * along)
        totals = others[0] + step_size * (others[1] + growth * others[2])
        level = totals[0:1] / totals[1:2]
        for x, y, z in local:
            charge_ref[x, y, z : z + 1, :] = 1000.0 * (
                answer[x, y, z, 0:1] - level * answer[x, y, z, 1:2]
            )
            for s in range(2):
                resid_ref[s, x, y, z : z + 1, :] = residual[x, y, z, s : s + 1]
        with jax.named_scope("drain"):
            all_of(sent, (send_sem.at[0], halo_recv.at[0])).wait_send()

    scratch = [
        pltpu.VMEM((3,) + cells + (atoms,), jnp.float32),
        pltpu.VMEM(cells + (atoms,), jnp.int32),
        None,
        pltpu.SMEM((types,), jnp.float32),
        pltpu.SMEM((types,), jnp.float32),
        pltpu.SMEM((types,), jnp.float32),
        pltpu.VMEM(width + (4, atoms), jnp.float32),
        pltpu.VMEM(width + (32, atoms), jnp.float32),
        pltpu.VMEM(width + (1, atoms), jnp.float32),
        pltpu.VMEM((tiles, 2, atoms, atoms), jnp.float32),
        pltpu.VMEM((len(STEPS), tiles, atoms), jnp.float32),
        pltpu.VMEM((tiles, len(STEPS), atoms, atoms), jnp.float32),
        pltpu.VMEM((tiles, 2, atoms, atoms), jnp.float32),
        pltpu.VMEM(width + (2, atoms), jnp.float32),
        pltpu.VMEM(width + (2, atoms), jnp.float32),
        pltpu.VMEM(width + (2, atoms), jnp.float32),
        pltpu.VMEM(cells + (2, atoms), jnp.float32),
    ]
    scratch += [pltpu.VMEM((ITERS, count, 1, atoms), jnp.float32) for count in group_sizes]
    scratch += [
        pltpu.SemaphoreType.DMA((6,)),
        pltpu.SemaphoreType.DMA((1,)),
        pltpu.SemaphoreType.DMA((len(brought),)),
        pltpu.SemaphoreType.DMA((ITERS, len(groups))),
        pltpu.SemaphoreType.REGULAR((2,)),
        pltpu.VMEM((sent, 1, atoms), jnp.float32),
    ]
    return kernel, scratch


def put_out(charge_in, resid_in, charge_ref, resid_ref, sems):
    copies = [
        pltpu.make_async_copy(charge_in, charge_ref, sems.at[0]),
        pltpu.make_async_copy(resid_in, resid_ref, sems.at[1]),
    ]
    for copy in copies:
        copy.start()
    for copy in copies:
        copy.wait()


def solution(mesh):
    sizes = {a: mesh.shape[a] for a in AXES}
    devices = sizes["gx"] * sizes["gy"] * sizes["gz"]
    groups = (AXES,) if devices <= 64 else tuple((a,) for a in AXES)

    def per_device(offsets, type_ids, neighbours, type_chi, type_eta, type_gamma):
        cells = offsets.shape[1:4]
        atoms = offsets.shape[4]
        types = type_chi.shape[0]
        kernel, scratch = make_kernel(sizes, groups, cells, atoms, types, 128)
        scratch[2] = pltpu.VMEM(neighbours.shape, jnp.int32)
        vmem = pl.BlockSpec(memory_space=pltpu.VMEM)
        hbm = pl.BlockSpec(memory_space=pltpu.HBM)
        pair = pl.pallas_call(
            kernel,
            out_shape=(
                jax.ShapeDtypeStruct(cells + (atoms,), jnp.float32),
                jax.ShapeDtypeStruct((2,) + cells + (atoms,), jnp.float32),
            ),
            in_specs=[hbm] * 6,
            out_specs=(vmem, vmem),
            scratch_shapes=scratch,
            compiler_params=pltpu.CompilerParams(
                collective_id=0, has_side_effects=True, vmem_limit_bytes=48 * 1024 * 1024
            ),
        )(*[pltpu.with_memory_space_constraint(v, pltpu.HBM) for v in (offsets, type_ids, neighbours, type_chi, type_eta, type_gamma)])
        return pl.pallas_call(
            put_out,
            out_shape=tuple(jax.ShapeDtypeStruct(v.shape, v.dtype) for v in pair),
            in_specs=[vmem] * 2,
            out_specs=(hbm, hbm),
            scratch_shapes=[pltpu.SemaphoreType.DMA((2,))],
        )(*[pltpu.with_memory_space_constraint(v, pltpu.VMEM) for v in pair])

    placed = (
        P(None, "gx", "gy", "gz", None),
        P("gx", "gy", "gz", None),
        P("gx", "gy", "gz", None),
        P(),
        P(),
        P(),
    )
    return jax.shard_map(
        per_device,
        mesh=mesh,
        in_specs=placed,
        out_specs=(P("gx", "gy", "gz", None), P(None, "gx", "gy", "gz", None)),
        check_vma=False,
    )
```
